128 devices in a mesh: stage: 1, data: 64 (over z, y, x), tp: 2 (over core).
Axes of the slice: x: 4, y: 4, z: 4, core: 2. Of those that a mesh axis runs over, the one named last changes fastest.
Arguments:
- weight: float32 [12, 576, 1536], P('stage', None, 'tp')
- momentum: float32 [12, 576, 1536], P('stage', None, 'tp')
- grad: bfloat16 [12, 64, 576, 1536], P('stage', 'data', None, 'tp')
Outputs:
- output 1: float32 [12, 576, 1536], P('stage', None, 'tp')
- output 2: float32 [12, 576, 1536], P('stage', None, 'tp')
All inputs are finite; a program needn't handle non-finite values.
Results may differ from the reference program's by a relative error of at most 0.0155555.
Values are sent between devices in bfloat16 or wider.
A program may use at most 1 GiB of HBM per device.

```python
import math
import jax
import jax.numpy as jnp
from jax import lax

LAYERS = 12
DATA = 64
M_ROWS = 576
N_COLS = 1536
NS_STEPS = 5
REGIONS = 16
MOMENTUM = 0.95
LEARN_RATE = 0.25
WEIGHT_DECAY = 0.1
COEF_A = 3.4445
COEF_B = -4.7750
COEF_C = 2.0315
NORM_EPS = 1e-7


def column_profile(key):
    tilt = jnp.linspace(-2.0, 2.0, N_COLS)
    jitter = 0.3 * jax.random.normal(key, (N_COLS,))
    return jnp.exp2(tilt + jitter)


def structured(key, lead):
    k_noise, k_left, k_right = jax.random.split(key, 3)
    noise = jax.random.normal(k_noise, lead + (M_ROWS, N_COLS))
    left = jax.random.normal(k_left, lead + (M_ROWS, REGIONS, 1))
    right = jax.random.normal(k_right, lead + (1, REGIONS, N_COLS // REGIONS))
    return noise + (left * right).reshape(lead + (M_ROWS, N_COLS))


def setup_inputs(seed: int = 0, part: int = 0) -> dict:
    key = jax.random.fold_in(jax.random.key(seed), part)
    k_w, k_m, k_g, k_mp, k_gp = jax.random.split(key, 5)
    weight = 0.02 * jax.random.normal(k_w, (LAYERS, M_ROWS, N_COLS))
    momentum = column_profile(k_mp) * structured(k_m, (LAYERS,))
    grad = math.sqrt(DATA) * column_profile(k_gp) * structured(k_g, (LAYERS, DATA))
    return {"weight": weight, "momentum": momentum, "grad": grad.astype(jnp.bfloat16)}


def ns_step(ortho):
    gram_mat = jnp.dot(ortho, ortho.T, preferred_element_type=jnp.float32).astype(jnp.bfloat16)
    square_mat = jnp.dot(gram_mat, gram_mat, preferred_element_type=jnp.float32)
    poly_mat = (COEF_B * gram_mat.astype(jnp.float32) + COEF_C * square_mat).astype(jnp.bfloat16)
    update = jnp.dot(poly_mat, ortho, preferred_element_type=jnp.float32)
    return (COEF_A * ortho.astype(jnp.float32) + update).astype(jnp.bfloat16)


def one_layer(layer_args):
    weight, momentum, grad = layer_args
    grad_mean = jnp.sum(grad.astype(jnp.float32), axis=0) / DATA
    new_mom = MOMENTUM * momentum + grad_mean
    nesterov = grad_mean + MOMENTUM * new_mom
    norm_value = jnp.sqrt(jnp.sum(nesterov * nesterov))
    ortho = (nesterov / (norm_value + NORM_EPS)).astype(jnp.bfloat16)
    ortho = lax.fori_loop(0, NS_STEPS, lambda step_idx, current: ns_step(current), ortho)
    rms_scale = 0.2 * math.sqrt(max(M_ROWS, N_COLS))
    new_weight = weight - LEARN_RATE * (rms_scale * ortho.astype(jnp.float32) + WEIGHT_DECAY * weight)
    return new_weight, new_mom


def reference(weight, momentum, grad):
    new_weight, new_momentum = lax.map(one_layer, (weight, momentum, grad))
    return new_weight, new_momentum
```

```python
import math
import jax
import jax.numpy as jnp
from jax import lax
from jax.sharding import PartitionSpec as P

MOMENTUM = 0.95
LEARN_RATE = 0.25
WEIGHT_DECAY = 0.1
COEF_A = 3.4445
COEF_B = -4.7750
COEF_C = 2.0315
NORM_EPS = 1e-7
NS_STEPS = 5


def to_tiles(arr):
    layers, rows, cols = arr.shape
    arr = arr.reshape(layers, rows // 8, 8, cols // 128, 128).transpose(0, 1, 3, 2, 4)
    return arr.reshape(layers * (rows // 8) * (cols // 128), 8, 128)


def from_tiles(tiles, layers, rows, cols):
    arr = tiles.reshape(layers, rows // 8, cols // 128, 8, 128).transpose(0, 1, 3, 2, 4)
    return arr.reshape(layers, rows, cols)


def dot_nn(lhs, rhs):
    return lax.dot_general(lhs, rhs, (((1,), (0,)), ((), ())), preferred_element_type=jnp.float32)


def dot_nt(lhs, rhs):
    return lax.dot_general(lhs, rhs, (((1,), (1,)), ((), ())), preferred_element_type=jnp.float32)


def solution(mesh):
    data_size = mesh.shape["data"]
    tp_size = mesh.shape["tp"]
    state_spec = P("stage", None, "tp")
    grad_spec = P("stage", "data", None, "tp")
    swap = [(0, 1), (1, 0)]

    def per_device(weight, momentum, grad):
        layers, rows, cols = weight.shape
        tiles_each = (rows // 8) * (cols // 128)
        share = layers * tiles_each // data_size
        data_idx = lax.axis_index("data")
        tp_idx = lax.axis_index("tp")

        grad_tiles = to_tiles(grad[:, 0].astype(jnp.float32))
        own = lax.psum_scatter(grad_tiles, "data", scatter_dimension=0, tiled=True) / data_size
        grad_mean = from_tiles(lax.all_gather(own, "data", axis=0, tiled=True), layers, rows, cols)
        new_mom = MOMENTUM * momentum + grad_mean

        first = (data_idx * share) // tiles_each
        last = (data_idx * share + share - 1) // tiles_each
        mine = jnp.where(tp_idx == 0, first, last)
        other = jnp.where(tp_idx == 0, last, first)

        def nesterov_of(which):
            mean = lax.dynamic_index_in_dim(grad_mean, which, 0, keepdims=False)
            mom = lax.dynamic_index_in_dim(momentum, which, 0, keepdims=False)
            return mean + MOMENTUM * (MOMENTUM * mom + mean)

        here = nesterov_of(mine)
        there = lax.ppermute(nesterov_of(other), "tp", swap)
        is_left = tp_idx == 0
        full = jnp.concatenate([jnp.where(is_left, here, there), jnp.where(is_left, there, here)], axis=1)
        norm = jnp.sqrt(jnp.sum(full * full))
        ortho = (full / (norm + NORM_EPS)).astype(jnp.bfloat16)
        for step_idx in range(NS_STEPS):
            gram_mat = dot_nt(ortho, ortho).astype(jnp.bfloat16)
            square_mat = dot_nn(gram_mat, gram_mat)
            poly_mat = (COEF_B * gram_mat.astype(jnp.float32) + COEF_C * square_mat).astype(jnp.bfloat16)
            update = dot_nn(poly_mat, ortho)
            ortho = (COEF_A * ortho.astype(jnp.float32) + update).astype(jnp.bfloat16)
        left, right = ortho[:, :cols], ortho[:, cols:]
        keep = jnp.where(is_left, left, right)
        got = lax.ppermute(jnp.where(is_left, right, left), "tp", swap)
        pair = jnp.stack([jnp.where(is_left, keep, got), jnp.where(is_left, got, keep)])
        piece = lax.dynamic_slice_in_dim(to_tiles(pair), data_idx * share - first * tiles_each, share, 0)
        ortho_all = from_tiles(lax.all_gather(piece, "data", axis=0, tiled=True), layers, rows, cols)
        rms_scale = 0.2 * math.sqrt(max(rows, cols * tp_size))
        new_weight = weight - LEARN_RATE * (rms_scale * ortho_all.astype(jnp.float32) + WEIGHT_DECAY * weight)
        return new_weight, new_mom

    return jax.shard_map(per_device, mesh=mesh, in_specs=(state_spec, state_spec, grad_spec), out_specs=(state_spec, state_spec), check_vma=False)
```

```python
import functools
import math
import jax
import jax.numpy as jnp
from jax import lax
from jax.experimental import pallas as pl
from jax.experimental.pallas import tpu as pltpu
from jax.sharding import PartitionSpec as P

MOMENTUM = 0.95
LEARN_RATE = 0.25
WEIGHT_DECAY = 0.1
COEF_A = 3.4445
COEF_B = -4.7750
COEF_C = 2.0315
NORM_EPS = 1e-7
NS_STEPS = 5

MESH = pl.DeviceIdType.MESH
SIDE = 4
PARTS = 3
STRIDES = (1, 4, 16)
KINDS = 6
PHASES = 6
SWAPS = 4


def dot_nn(lhs, rhs):
    return lax.dot_general(lhs, rhs, (((1,), (0,)), ((), ())), preferred_element_type=jnp.float32)


def dot_nt(lhs, rhs):
    return lax.dot_general(lhs, rhs, (((1,), (1,)), ((), ())), preferred_element_type=jnp.float32)


def kernel(rows, cols, data_size, grad_ref, mom_ref, mean_ref, ortho_ref, raw_in, raw_relay, raw_own, sum_line, line_in,
           line_relay, plane, mean_own, mom_own, nest, nest_in, x_buf, gram_buf, poly_buf, x_half, send_sem, recv_sem,
           local_sem):
    data_idx = lax.axis_index("data")
    tp_idx = lax.axis_index("tp")
    partner = {"tp": 1 - tp_idx}
    half = rows // 2
    quarter = rows // SIDE
    eighth = quarter // 2

    coord, plus, minus = [], [], []
    for stride in STRIDES:
        here = lax.rem(lax.div(data_idx, stride), SIDE)
        coord.append(here)
        plus.append({"data": data_idx + (lax.rem(here + 1, SIDE) - here) * stride})
        minus.append({"data": data_idx + (lax.rem(here + SIDE - 1, SIDE) - here) * stride})

    def step_of(axis, distance):
        return lax.rem(coord[axis] + distance, SIDE)

    def axes_of(part):
        return part, (part + 1) % PARTS, (part + 2) % PARTS

    def remote(src, dst, index, device):
        return pltpu.make_async_remote_copy(src_ref=src, dst_ref=dst, send_sem=send_sem.at[index],
                                            recv_sem=recv_sem.at[index], device_id=device, device_id_type=MESH)

    def base_of(phase, part):
        return (phase * PARTS + part) * KINDS

    def local(src, dst, index):
        return pltpu.make_async_copy(src, dst, local_sem.at[index])

    def spread(phase, part, axis, block, height, relay, landing):
        base = base_of(phase, part)
        mid = height // 2
        far = step_of(axis, 2)
        return [
            remote(block(far, 0, mid), relay.at[0], base + 0, plus[axis]),
            remote(block(far, mid, mid), relay.at[1], base + 1, minus[axis]),
            remote(block(step_of(axis, 1), 0, height), landing.at[0], base + 2, plus[axis]),
            remote(block(step_of(axis, 3), 0, height), landing.at[1], base + 3, minus[axis]),
            remote(relay.at[0], landing.at[2, pl.ds(0, mid)], base + 4, plus[axis]),
            remote(relay.at[1], landing.at[2, pl.ds(mid, mid)], base + 5, minus[axis]),
        ]

    def gather(phase, part, axis, own, slot):
        base = base_of(phase, part)
        here = coord[axis]
        left, right = step_of(axis, 3), step_of(axis, 1)
        return [
            remote(own(0), slot(here, 0), base + 0, plus[axis]),
            remote(own(1), slot(here, 1), base + 1, minus[axis]),
            remote(own(1), slot(here, 1), base + 2, plus[axis]),
            remote(own(0), slot(here, 0), base + 3, minus[axis]),
            remote(slot(left, 0), slot(left, 0), base + 4, plus[axis]),
            remote(slot(right, 1), slot(right, 1), base + 5, minus[axis]),
        ]

    def launch(copies):
        for copy in copies[:4]:
            copy.start()

    def forward(copies):
        copies[0].wait_recv()
        copies[4].start()
        copies[1].wait_recv()
        copies[5].start()

    def arrive(copies):
        for copy in copies[2:]:
            copy.wait_recv()

    def over_rows(count, chunk, body):
        def run(index, carry):
            body(pl.ds(pl.multiple_of(index * chunk, chunk), chunk))
            return carry
        lax.fori_loop(0, count // chunk, run, 0)

    fetch_raw, fetch_mom = [], []
    for part in range(PARTS):
        mine = part * SIDE + step_of(part, 0)
        fetch_raw.append(local(grad_ref.at[mine], raw_own.at[part], part))
        fetch_mom.append(local(mom_ref.at[mine], mom_own.at[part], PARTS + part))
    for fetch in fetch_raw + fetch_mom:
        fetch.start()

    barrier = pltpu.get_barrier_semaphore()
    for device in plus + minus + [partner]:
        pl.semaphore_signal(barrier, inc=1, device_id=device, device_id_type=MESH)
    pl.semaphore_wait(barrier, 2 * PARTS + 1)

    copies1, copies2, copies3, copies4, copies5, copies6 = [], [], [], [], [], []
    for part in range(PARTS):
        copies1.append(spread(0, part, part, lambda j, at, size, part=part: grad_ref.at[part * SIDE + j, pl.ds(at, size)],
                              rows, raw_relay.at[part], raw_in.at[part]))
        launch(copies1[part])
    for part in range(PARTS):
        forward(copies1[part])

    for part in range(PARTS):
        fetch_raw[part].wait()
        arrive(copies1[part])

        def add_line(at, part=part):
            total = raw_own[part, at].astype(jnp.float32) + raw_in[part, 0, at].astype(jnp.float32)
            total = total + raw_in[part, 1, at].astype(jnp.float32)
            sum_line[part, at] = total + raw_in[part, 2, at].astype(jnp.float32)

        over_rows(rows, 16, add_line)
        axis = axes_of(part)[1]

        def quarter_block(j, at, size, part=part):
            return sum_line.at[part, pl.ds(pl.multiple_of(j * quarter + at, 8), size)]

        copies2.append(spread(1, part, axis, quarter_block, quarter, line_relay.at[part], line_in.at[part]))
        launch(copies2[part])
    for part in range(PARTS):
        forward(copies2[part])

    for part in range(PARTS):
        arrive(copies2[part])
        axis_b, axis_c = axes_of(part)[1:]

        def add_plane(at, part=part, axis_b=axis_b, axis_c=axis_c):
            own_at = pl.ds(pl.multiple_of(coord[axis_b] * quarter + at.start, 8), at.size)
            plane[part, coord[axis_c], at] = (sum_line[part, own_at] + line_in[part, 0, at]) + (
                line_in[part, 1, at] + line_in[part, 2, at])

        over_rows(quarter, 16, add_plane)

        def plane_slot(slot, which, part=part):
            return plane.at[part, slot, pl.ds(which * eighth, eighth)]

        copies3.append(gather(2, part, axis_c, lambda which, slot=plane_slot, axis=axis_c: slot(coord[axis], which), plane_slot))
        launch(copies3[part])
    for part in range(PARTS):
        forward(copies3[part])

    for part in range(PARTS):
        arrive(copies3[part])
        axis_b = axes_of(part)[1]

        def add_cube(at, part=part, axis_b=axis_b):
            own_at = pl.ds(pl.multiple_of(coord[axis_b] * quarter + at.start, 8), at.size)
            total = (plane[part, 0, at] + plane[part, 1, at]) + (plane[part, 2, at] + plane[part, 3, at])
            mean_own[part, own_at] = total * (1.0 / data_size)

        over_rows(quarter, 16, add_cube)

        def mean_slot(slot, which, part=part):
            return mean_own.at[part, pl.ds(pl.multiple_of(slot * quarter + which * eighth, 8), eighth)]

        copies4.append(gather(3, part, axis_b, lambda which, slot=mean_slot, axis=axis_b: slot(coord[axis], which), mean_slot))
        launch(copies4[part])
    for part in range(PARTS):
        forward(copies4[part])

    for part in range(PARTS):
        arrive(copies4[part])
        mine = part * SIDE + step_of(part, 0)

        def out_slot(slot, which, part=part):
            return mean_ref.at[part * SIDE + slot, pl.ds(which * half, half)]

        copies5.append(gather(4, part, part, lambda which, part=part: mean_own.at[part, pl.ds(which * half, half)], out_slot))
        launch(copies5[part])
        local(mean_own.at[part], mean_ref.at[mine], 2 * PARTS + part).start()

    swap_base = PHASES * PARTS * KINDS
    for part in range(PARTS):
        fetch_mom[part].wait()

        def nesterov(at, part=part):
            mean = mean_own[part, at]
            nest[part, at] = mean + MOMENTUM * (MOMENTUM * mom_own[part, at] + mean)

        over_rows(rows, 16, nesterov)
    give_first = remote(nest.at[1 - tp_idx], nest_in.at[0], swap_base, partner)
    give_first.start()
    give_second = remote(nest.at[2], nest_in.at[1], swap_base + 1, partner)

    @pl.when(tp_idx == 1)
    def _():
        give_second.start()

    def orthogonalise(part, which):
        def squares(index, total):
            at = pl.ds(pl.multiple_of(index * 8, 8), 8)
            own, other = nest[part, at], nest_in[which, at]
            return total + (own * own + other * other)

        total = lax.fori_loop(0, rows // 8, squares, jnp.zeros((8, cols), jnp.float32))
        scale = 1.0 / (jnp.sqrt(jnp.sum(total, keepdims=True)) + NORM_EPS)

        def normalise(at):
            x_buf[0, at, pl.ds(0, cols)] = (nest[part, at] * scale).astype(jnp.bfloat16)
            x_buf[0, at, pl.ds(cols, cols)] = (nest_in[which, at] * scale).astype(jnp.bfloat16)

        over_rows(rows, 16, normalise)

        def newton(step, carry):
            now = lax.rem(step, 2)
            later = 1 - now
            gram_buf[...] = dot_nt(x_buf[now], x_buf[now]).astype(jnp.bfloat16)
            square = dot_nn(gram_buf[...], gram_buf[...])
            poly_buf[...] = (COEF_B * gram_buf[...].astype(jnp.float32) + COEF_C * square).astype(jnp.bfloat16)
            for at in range(0, 2 * cols, cols // 3):
                strip = x_buf[now, :, pl.ds(at, cols // 3)]
                update = dot_nn(poly_buf[...], strip)
                x_buf[later, :, pl.ds(at, cols // 3)] = (COEF_A * strip.astype(jnp.float32) + update).astype(jnp.bfloat16)
            return carry

        lax.fori_loop(0, NS_STEPS, newton, 0)

    final = NS_STEPS % 2

    def keep_half(part):
        def move(at):
            x_half[part, at] = x_buf[final, at, pl.ds(0, cols)]
        over_rows(rows, 16, move)

    give_first.wait_recv()
    orthogonalise(tp_idx, 0)
    swap_x = remote(x_buf.at[final, :, pl.ds(cols, cols)], x_half.at[tp_idx], swap_base + 2, partner)
    swap_x.start()
    for part in range(PARTS):
        forward(copies5[part])
    keep_half(tp_idx)
    swap_x.wait()

    def ortho_gather(part):
        mine = part * SIDE + step_of(part, 0)

        def slot(index, which):
            return ortho_ref.at[part * SIDE + index, pl.ds(which * half, half)]

        copies = gather(5, part, part, lambda which: x_half.at[part, pl.ds(which * half, half)], slot)
        launch(copies)
        local(x_half.at[part], ortho_ref.at[mine], 3 * PARTS + part).start()
        return copies

    copies6.append(ortho_gather(0))
    copies6.append(ortho_gather(1))

    give_x = remote(x_buf.at[final, :, pl.ds(cols, cols)], x_half.at[2], swap_base + 3, partner)

    @pl.when(tp_idx == 0)
    def _():
        give_second.wait_recv()
        orthogonalise(2, 1)
        give_x.start()
        keep_half(2)
        give_x.wait_send()

    @pl.when(tp_idx == 1)
    def _():
        forward(copies6[0])
        forward(copies6[1])
        give_x.wait_recv()
        give_second.wait_send()

    copies6.append(ortho_gather(2))

    @pl.when(tp_idx == 0)
    def _():
        forward(copies6[0])
        forward(copies6[1])

    forward(copies6[2])
    for part in range(PARTS):
        arrive(copies5[part])
        arrive(copies6[part])
        mine = part * SIDE + step_of(part, 0)
        local(mean_own.at[part], mean_ref.at[mine], 2 * PARTS + part).wait()
        local(x_half.at[part], ortho_ref.at[mine], 3 * PARTS + part).wait()
    give_first.wait_send()
    for copies in copies1 + copies2 + copies3 + copies4 + copies5 + copies6:
        for copy in copies:
            copy.wait_send()


def solution(mesh):
    data_size = mesh.shape["data"]
    tp_size = mesh.shape["tp"]
    state_spec = P("stage", None, "tp")
    grad_spec = P("stage", "data", None, "tp")

    def per_device(weight, momentum, grad):
        layers, rows, cols = weight.shape
        quarter = rows // SIDE
        copies = PHASES * PARTS * KINDS + SWAPS
        bf16, f32 = jnp.bfloat16, jnp.float32
        mean, ortho = pl.pallas_call(
            functools.partial(kernel, rows, cols, data_size),
            out_shape=(jax.ShapeDtypeStruct((layers, rows, cols), f32), jax.ShapeDtypeStruct((layers, rows, cols), bf16)),
            in_specs=[pl.BlockSpec(memory_space=pl.ANY)] * 2,
            out_specs=(pl.BlockSpec(memory_space=pl.ANY),) * 2,
            scratch_shapes=[
                pltpu.VMEM((PARTS, 3, rows, cols), bf16),
                pltpu.VMEM((PARTS, 2, rows // 2, cols), bf16),
                pltpu.VMEM((PARTS, rows, cols), bf16),
                pltpu.VMEM((PARTS, rows, cols), f32),
                pltpu.VMEM((PARTS, 3, quarter, cols), f32),
                pltpu.VMEM((PARTS, 2, quarter // 2, cols), f32),
                pltpu.VMEM((PARTS, SIDE, quarter, cols), f32),
                pltpu.VMEM((PARTS, rows, cols), f32),
                pltpu.VMEM((PARTS, rows, cols), f32),
                pltpu.VMEM((PARTS, rows, cols), f32),
                pltpu.VMEM((2, rows, cols), f32),
                pltpu.VMEM((2, rows, tp_size * cols), bf16),
                pltpu.VMEM((rows, rows), bf16),
                pltpu.VMEM((rows, rows), bf16),
                pltpu.VMEM((PARTS, rows, cols), bf16),
                pltpu.SemaphoreType.DMA((copies,)),
                pltpu.SemaphoreType.DMA((copies,)),
                pltpu.SemaphoreType.DMA((4 * PARTS,)),
            ],
            compiler_params=pltpu.CompilerParams(collective_id=0, has_side_effects=True, vmem_limit_bytes=67043328),
        )(grad.reshape(layers, rows, cols), momentum)
        new_mom = MOMENTUM * momentum + mean
        rms_scale = 0.2 * math.sqrt(max(rows, cols * tp_size))
        new_weight = weight - LEARN_RATE * (rms_scale * ortho.astype(f32) + WEIGHT_DECAY * weight)
        return new_weight, new_mom

    return jax.shard_map(per_device, mesh=mesh, in_specs=(state_spec, state_spec, grad_spec), out_specs=(state_spec, state_spec), check_vma=False)
```

```python
import functools
import math
import jax
import jax.numpy as jnp
from jax import lax
from jax.experimental import pallas as pl
from jax.experimental.pallas import tpu as pltpu
from jax.sharding import PartitionSpec as P

MOMENTUM = 0.95
LEARN_RATE = 0.25
WEIGHT_DECAY = 0.1
COEF_A = 3.4445
COEF_B = -4.7750
COEF_C = 2.0315
NORM_EPS = 1e-7
NS_STEPS = 5

MESH = pl.DeviceIdType.MESH
SIDE = 4
PARTS = 3
STRIDES = (1, 4, 16)
KINDS = 6
PHASES = 6
SWAPS = 4
VMEM_KERNEL = 22 * 1024 * 1024
VMEM_FLUSH = 1024 * 1024
ORDER = (0, 3, 1, 2)


def dot_nn(lhs, rhs):
    return lax.dot_general(lhs, rhs, (((1,), (0,)), ((), ())), preferred_element_type=jnp.float32)


def dot_nt(lhs, rhs):
    return lax.dot_general(lhs, rhs, (((1,), (1,)), ((), ())), preferred_element_type=jnp.float32)


def kernel(rows, cols, data_size, rms_scale, grad_ref, mom_ref, weight_ref, held, ortho_all, x_buf, gram_buf, poly_buf,
           nest_in, send_sem, recv_sem, local_sem):
    data_idx = lax.axis_index("data")
    tp_idx = lax.axis_index("tp")
    partner = {"tp": 1 - tp_idx}
    half = rows // 2
    quarter = rows // SIDE
    eighth = quarter // 2
    layers = PARTS * SIDE
    mom_out = held.at[pl.ds(0, layers)]
    weight_out = held.at[pl.ds(layers, layers)]

    def raw_in(part, slot):
        return ortho_all.at[part * 3 + slot]

    def raw_relay(part, way):
        return ortho_all.at[3 * PARTS + part, pl.ds(way * half, half)]

    def raw_own(part):
        return x_buf.at[part // 2, :, pl.ds(part % 2 * cols, cols)]

    def sum_line(part):
        return weight_out.at[part]

    def line_in(part, slot):
        return weight_out.at[PARTS + part, pl.ds(slot * quarter, quarter)]

    def line_relay(part, way):
        return weight_out.at[PARTS + part, pl.ds(3 * quarter + way * eighth, eighth)]

    def plane(part, slot):
        return weight_out.at[2 * PARTS + part, pl.ds(pl.multiple_of(slot * quarter, 8), quarter)]

    def mom_own(part):
        return weight_out.at[3 * PARTS + part]

    def nest(part):
        return weight_out.at[part]

    coord, plus, minus = [], [], []
    for stride in STRIDES:
        here = lax.rem(lax.div(data_idx, stride), SIDE)
        coord.append(here)
        plus.append({"data": data_idx + (lax.rem(here + 1, SIDE) - here) * stride})
        minus.append({"data": data_idx + (lax.rem(here + SIDE - 1, SIDE) - here) * stride})

    def step_of(axis, distance):
        return lax.rem(coord[axis] + distance, SIDE)

    def layer_of(part, distance):
        return part * SIDE + step_of(part, distance)

    def axes_of(part):
        return part, (part + 1) % PARTS, (part + 2) % PARTS

    def remote(src, dst, index, device):
        return pltpu.make_async_remote_copy(src_ref=src, dst_ref=dst, send_sem=send_sem.at[index],
                                            recv_sem=recv_sem.at[index], device_id=device, device_id_type=MESH)

    def base_of(phase, part):
        return (phase * PARTS + part) * KINDS

    def local(src, dst, index):
        return pltpu.make_async_copy(src, dst, local_sem.at[index])

    def spread(phase, part, axis, block, height, relay, landing):
        base = base_of(phase, part)
        mid = height // 2
        far = step_of(axis, 2)
        return [
            remote(block(far, 0, mid), relay(part, 0), base + 0, plus[axis]),
            remote(block(far, mid, mid), relay(part, 1), base + 1, minus[axis]),
            remote(block(step_of(axis, 1), 0, height), landing(part, 0), base + 2, plus[axis]),
            remote(block(step_of(axis, 3), 0, height), landing(part, 1), base + 3, minus[axis]),
            remote(relay(part, 0), landing(part, 2).at[pl.ds(0, mid)], base + 4, plus[axis]),
            remote(relay(part, 1), landing(part, 2).at[pl.ds(mid, mid)], base + 5, minus[axis]),
        ]

    def gather(phase, part, axis, slot):
        base = base_of(phase, part)
        here = coord[axis]
        left, right = step_of(axis, 3), step_of(axis, 1)
        return [
            remote(slot(here, 0), slot(here, 0), base + 0, plus[axis]),
            remote(slot(here, 1), slot(here, 1), base + 1, minus[axis]),
            remote(slot(here, 1), slot(here, 1), base + 2, plus[axis]),
            remote(slot(here, 0), slot(here, 0), base + 3, minus[axis]),
            remote(slot(left, 0), slot(left, 0), base + 4, plus[axis]),
            remote(slot(right, 1), slot(right, 1), base + 5, minus[axis]),
        ]

    def launch(copies):
        for copy in copies[:4]:
            copy.start()

    def forward(copies):
        copies[0].wait_recv()
        copies[4].start()
        copies[1].wait_recv()
        copies[5].start()

    def arrive(copies):
        for copy in copies[2:]:
            copy.wait_recv()

    def sent(copies):
        for copy in copies:
            copy.wait_send()

    def over_rows(count, chunk, body):
        def run(index, carry):
            body(pl.ds(pl.multiple_of(index * chunk, chunk), chunk))
            return carry
        lax.fori_loop(0, count // chunk, run, 0)

    fetch_raw, fetch_mom = [], []
    for part in range(PARTS):
        fetch_raw.append(local(grad_ref.at[layer_of(part, 0)], raw_own(part), part))
        fetch_mom.append(local(mom_ref.at[layer_of(part, 0)], mom_own(part), PARTS + part))
    for fetch in fetch_raw + fetch_mom:
        fetch.start()

    barrier = pltpu.get_barrier_semaphore()
    for device in plus + minus + [partner]:
        pl.semaphore_signal(barrier, inc=1, device_id=device, device_id_type=MESH)
    pl.semaphore_wait(barrier, 2 * PARTS + 1)

    copies1, copies2, copies3, copies4, copies5, copies6 = [], [], [], [], [], []
    for part in range(PARTS):
        def raw_block(j, at, size, part=part):
            return grad_ref.at[part * SIDE + j, pl.ds(at, size)]

        copies1.append(spread(0, part, part, raw_block, rows, raw_relay, raw_in))
        launch(copies1[part])
    for part in range(PARTS):
        forward(copies1[part])

    for part in range(PARTS):
        fetch_raw[part].wait()
        arrive(copies1[part])

        def add_line(at, part=part):
            total = raw_own(part)[at].astype(jnp.float32) + raw_in(part, 0)[at].astype(jnp.float32)
            total = total + raw_in(part, 1)[at].astype(jnp.float32)
            sum_line(part)[at] = total + raw_in(part, 2)[at].astype(jnp.float32)

        over_rows(rows, 16, add_line)

        def quarter_block(j, at, size, part=part):
            return sum_line(part).at[pl.ds(pl.multiple_of(j * quarter + at, 8), size)]

        copies2.append(spread(1, part, axes_of(part)[1], quarter_block, quarter, line_relay, line_in))
        launch(copies2[part])
    for part in range(PARTS):
        forward(copies2[part])

    for part in range(PARTS):
        arrive(copies2[part])
        axis_b, axis_c = axes_of(part)[1:]

        def add_plane(at, part=part, axis_b=axis_b, axis_c=axis_c):
            own_at = pl.ds(pl.multiple_of(coord[axis_b] * quarter + at.start, 8), at.size)
            plane(part, coord[axis_c])[at] = (sum_line(part)[own_at] + line_in(part, 0)[at]) + (
                line_in(part, 1)[at] + line_in(part, 2)[at])

        over_rows(quarter, 16, add_plane)

        def plane_slot(slot, which, part=part):
            return plane(part, slot).at[pl.ds(which * eighth, eighth)]

        copies3.append(gather(2, part, axis_c, plane_slot))
        launch(copies3[part])
    for part in range(PARTS):
        forward(copies3[part])

    for part in range(PARTS):
        arrive(copies3[part])
        axis_b = axes_of(part)[1]

        def add_cube(at, part=part, axis_b=axis_b):
            own_at = pl.ds(pl.multiple_of(coord[axis_b] * quarter + at.start, 8), at.size)
            total = (plane(part, 0)[at] + plane(part, 1)[at]) + (plane(part, 2)[at] + plane(part, 3)[at])
            mom_out[layer_of(part, 0), own_at] = total * (1.0 / data_size)

        over_rows(quarter, 16, add_cube)

        def mean_slot(slot, which, part=part):
            return mom_out.at[layer_of(part, 0), pl.ds(pl.multiple_of(slot * quarter + which * eighth, 8), eighth)]

        copies4.append(gather(3, part, axis_b, mean_slot))
        launch(copies4[part])
    for part in range(PARTS):
        forward(copies4[part])
    for part in range(PARTS):
        sent(copies1[part])
        sent(copies2[part])
        sent(copies3[part])

    for part in range(PARTS):
        arrive(copies4[part])

        def mean_block(slot, which, part=part):
            return mom_out.at[part * SIDE + slot, pl.ds(which * half, half)]

        copies5.append(gather(4, part, part, mean_block))
        launch(copies5[part])

    swap_base = PHASES * PARTS * KINDS
    for part in range(PARTS):
        fetch_mom[part].wait()

        def nesterov(at, part=part):
            mean = mom_out[layer_of(part, 0), at]
            nest(part)[at] = mean + MOMENTUM * (MOMENTUM * mom_own(part)[at] + mean)

        over_rows(rows, 16, nesterov)
    give_first = remote(weight_out.at[1 - tp_idx], nest_in.at[0], swap_base, partner)
    give_first.start()
    give_second = remote(nest(2), nest_in.at[1], swap_base + 1, partner)

    @pl.when(tp_idx == 1)
    def _():
        give_second.start()

    weight_base = 2 * PARTS
    fetch_weight = [local(weight_ref.at[layer], weight_out.at[layer], weight_base + layer) for layer in range(layers)]
    for fetch in fetch_weight[PARTS:]:
        fetch.start()

    def orthogonalise(part, which):
        def squares(index, total):
            at = pl.ds(pl.multiple_of(index * 8, 8), 8)
            own, other = weight_out[part, at], nest_in[which, at]
            return total + (own * own + other * other)

        total = lax.fori_loop(0, rows // 8, squares, jnp.zeros((8, cols), jnp.float32))
        scale = 1.0 / (jnp.sqrt(jnp.sum(total, keepdims=True)) + NORM_EPS)

        def normalise(at):
            x_buf[0, at, pl.ds(0, cols)] = (weight_out[part, at] * scale).astype(jnp.bfloat16)
            x_buf[0, at, pl.ds(cols, cols)] = (nest_in[which, at] * scale).astype(jnp.bfloat16)

        over_rows(rows, 16, normalise)

        def newton(step, carry):
            now = lax.rem(step, 2)
            later = 1 - now
            gram_buf[...] = dot_nt(x_buf[now], x_buf[now]).astype(jnp.bfloat16)
            square = dot_nn(gram_buf[...], gram_buf[...])
            poly_buf[...] = (COEF_B * gram_buf[...].astype(jnp.float32) + COEF_C * square).astype(jnp.bfloat16)
            for at in range(0, 2 * cols, cols // 3):
                strip = x_buf[now, :, pl.ds(at, cols // 3)]
                update = dot_nn(poly_buf[...], strip)
                x_buf[later, :, pl.ds(at, cols // 3)] = (COEF_A * strip.astype(jnp.float32) + update).astype(jnp.bfloat16)
            return carry

        lax.fori_loop(0, NS_STEPS, newton, 0)

    final = NS_STEPS % 2
    first_layer = jnp.where(tp_idx == 0, layer_of(0, 0), layer_of(1, 0))

    def keep_half(layer):
        def move(at):
            ortho_all[layer, at] = x_buf[final, at, pl.ds(0, cols)]
        over_rows(rows, 16, move)

    def ortho_gather(part):
        def slot(index, which):
            return ortho_all.at[part * SIDE + index, pl.ds(which * half, half)]

        copies6.append(gather(5, part, part, slot))
        launch(copies6[part])

    give_first.wait_recv()
    orthogonalise(tp_idx, 0)
    swap_x = remote(x_buf.at[final, :, pl.ds(cols, cols)], ortho_all.at[first_layer], swap_base + 2, partner)
    swap_x.start()
    for part in range(PARTS):
        forward(copies5[part])
    keep_half(first_layer)
    swap_x.wait()
    ortho_gather(0)
    ortho_gather(1)

    give_x = remote(x_buf.at[final, :, pl.ds(cols, cols)], ortho_all.at[layer_of(2, 0)], swap_base + 3, partner)

    @pl.when(tp_idx == 0)
    def _():
        give_second.wait_recv()
        orthogonalise(2, 1)
        give_x.start()
        keep_half(layer_of(2, 0))
        give_x.wait_send()

    @pl.when(tp_idx == 1)
    def _():
        give_x.wait_recv()
        give_second.wait_send()

    ortho_gather(2)
    give_first.wait_send()
    for fetch in fetch_weight[:PARTS]:
        fetch.start()

    stream_base = weight_base + layers
    turns = [(part, distance) for distance in ORDER for part in range(PARTS)]
    fetch_turn = [local(mom_ref.at[layer_of(*turn)], nest_in.at[index % 2], stream_base + index)
                  for index, turn in enumerate(turns)]
    fetch_turn[0].start()
    fetch_turn[1].start()
    for index, (part, distance) in enumerate(turns):
        if distance == 0:
            sent(copies4[part])
            sent(copies5[part][:4])
        elif distance == 3:
            copies5[part][2].wait_recv()
            copies5[part][4].wait_send()
        elif distance == 1:
            copies5[part][3].wait_recv()
            copies5[part][5].wait_send()
        else:
            copies5[part][4].wait_recv()
            copies5[part][5].wait_recv()
        fetch_turn[index].wait()
        layer = layer_of(part, distance)

        def momentum(at, layer=layer, index=index):
            mom_out[layer, at] = MOMENTUM * nest_in[index % 2, at] + mom_out[layer, at]

        over_rows(rows, 16, momentum)
        if index + 2 < len(turns):
            fetch_turn[index + 2].start()

    for part in range(PARTS):
        forward(copies6[part])
    for fetch in fetch_weight:
        fetch.wait()
    for part, distance in turns:
        if distance == 3:
            copies6[part][2].wait_recv()
        elif distance == 1:
            copies6[part][3].wait_recv()
        elif distance == 2:
            copies6[part][4].wait_recv()
            copies6[part][5].wait_recv()
        layer = layer_of(part, distance)

        def descend(at, layer=layer):
            weight = weight_out[layer, at]
            ortho = ortho_all[layer, at].astype(jnp.float32)
            weight_out[layer, at] = weight - LEARN_RATE * (rms_scale * ortho + WEIGHT_DECAY * weight)

        over_rows(rows, 16, descend)
    for part in range(PARTS):
        sent(copies6[part])


def flush(held, mom_ref, weight_ref, sem):
    layers = mom_ref.shape[0]
    copies = []
    for layer in range(layers):
        copies.append(pltpu.make_async_copy(held.at[layer], mom_ref.at[layer], sem.at[layer]))
        copies.append(pltpu.make_async_copy(held.at[layers + layer], weight_ref.at[layer], sem.at[layers + layer]))
    for copy in copies:
        copy.start()
    for copy in copies:
        copy.wait()


def solution(mesh):
    data_size = mesh.shape["data"]
    tp_size = mesh.shape["tp"]
    state_spec = P("stage", None, "tp")
    grad_spec = P("stage", "data", None, "tp")

    def per_device(weight, momentum, grad):
        layers, rows, cols = weight.shape
        copies = PHASES * PARTS * KINDS + SWAPS
        rms_scale = 0.2 * math.sqrt(max(rows, cols * tp_size))
        bf16, f32 = jnp.bfloat16, jnp.float32
        in_hbm = pl.BlockSpec(memory_space=pltpu.HBM)
        in_vmem = pl.BlockSpec(memory_space=pltpu.VMEM)
        held = pl.pallas_call(
            functools.partial(kernel, rows, cols, data_size, rms_scale),
            out_shape=pltpu.VMEM((2 * layers, rows, cols), f32),
            in_specs=[in_hbm] * 3,
            out_specs=in_vmem,
            scratch_shapes=[
                pltpu.VMEM((layers, rows, cols), bf16),
                pltpu.VMEM((2, rows, tp_size * cols), bf16),
                pltpu.VMEM((rows, rows), bf16),
                pltpu.VMEM((rows, rows), bf16),
                pltpu.VMEM((2, rows, cols), f32),
                pltpu.SemaphoreType.DMA((copies,)),
                pltpu.SemaphoreType.DMA((copies,)),
                pltpu.SemaphoreType.DMA((2 * PARTS + 2 * layers,)),
            ],
            compiler_params=pltpu.CompilerParams(collective_id=0, has_side_effects=True, vmem_limit_bytes=VMEM_KERNEL),
        )(grad.reshape(layers, rows, cols), momentum, weight)
        new_mom, new_weight = pl.pallas_call(
            flush,
            out_shape=(jax.ShapeDtypeStruct((layers, rows, cols), f32),) * 2,
            in_specs=[in_vmem],
            out_specs=(in_hbm,) * 2,
            scratch_shapes=[pltpu.SemaphoreType.DMA((2 * layers,))],
            compiler_params=pltpu.CompilerParams(vmem_limit_bytes=VMEM_FLUSH),
        )(held)
        return new_weight, new_mom

    return jax.shard_map(per_device, mesh=mesh, in_specs=(state_spec, state_spec, grad_spec), out_specs=(state_spec, state_spec), check_vma=False)
```

```python
import functools
import math
import jax
import jax.numpy as jnp
from jax import lax
from jax.experimental import pallas as pl
from jax.experimental.pallas import tpu as pltpu
from jax.sharding import PartitionSpec as P

MOMENTUM = 0.95
LEARN_RATE = 0.25
WEIGHT_DECAY = 0.1
COEF_A = 3.4445
COEF_B = -4.7750
COEF_C = 2.0315
NORM_EPS = 1e-7
NS_STEPS = 5

MESH = pl.DeviceIdType.MESH
SIDE = 4
PARTS = 3
STRIDES = (1, 4, 16)
KINDS = 6
PHASES = 6
CHUNKS = 2
SWAPS = 4
VMEM_KERNEL = 22 * 1024 * 1024
VMEM_FLUSH = 1024 * 1024
ORDER = (0, 3, 1, 2)


def dot_nn(lhs, rhs):
    return lax.dot_general(lhs, rhs, (((1,), (0,)), ((), ())), preferred_element_type=jnp.float32)


def dot_nt(lhs, rhs):
    return lax.dot_general(lhs, rhs, (((1,), (1,)), ((), ())), preferred_element_type=jnp.float32)


def kernel(rows, cols, data_size, rms_scale, grad_ref, mom_ref, weight_ref, held, ortho_all, x_buf, gram_buf, poly_buf,
           nest_in, send_sem, recv_sem, local_sem):
    data_idx = lax.axis_index("data")
    tp_idx = lax.axis_index("tp")
    partner = {"tp": 1 - tp_idx}
    half = rows // 2
    quarter = rows // SIDE
    eighth = quarter // 2
    layers = PARTS * SIDE
    mom_out = held.at[pl.ds(0, layers)]
    weight_out = held.at[pl.ds(layers, layers)]

    width = cols // CHUNKS

    def columns(chunk, start=0):
        return pl.ds(start + chunk * width, width)

    def raw_in(part, slot, chunk):
        return ortho_all.at[part * 3 + slot, :, columns(chunk)]

    def raw_relay(part, way, chunk):
        return ortho_all.at[3 * PARTS + part, pl.ds(way * half, half), columns(chunk)]

    def raw_own(part, chunk):
        return x_buf.at[part // 2, :, columns(chunk, part % 2 * cols)]

    def sum_line(part, chunk):
        return weight_out.at[part, :, columns(chunk)]

    def line_in(part, slot, chunk):
        return weight_out.at[PARTS + part, pl.ds(slot * quarter, quarter), columns(chunk)]

    def line_relay(part, way, chunk):
        return weight_out.at[PARTS + part, pl.ds(2 * quarter + way * eighth, eighth), columns(chunk)]

    def plane(part, slot, chunk):
        return weight_out.at[2 * PARTS + part, pl.ds(pl.multiple_of(slot * quarter, 8), quarter), columns(chunk)]

    def mom_own(part):
        return weight_out.at[3 * PARTS + part]

    def nest(part):
        return weight_out.at[part]

    coord, plus, minus = [], [], []
    for stride in STRIDES:
        here = lax.rem(lax.div(data_idx, stride), SIDE)
        coord.append(here)
        plus.append({"data": data_idx + (lax.rem(here + 1, SIDE) - here) * stride})
        minus.append({"data": data_idx + (lax.rem(here + SIDE - 1, SIDE) - here) * stride})

    def step_of(axis, distance):
        return lax.rem(coord[axis] + distance, SIDE)

    def layer_of(part, distance):
        return part * SIDE + step_of(part, distance)

    def axes_of(part):
        return part, (part + 1) % PARTS, (part + 2) % PARTS

    def remote(src, dst, index, device):
        return pltpu.make_async_remote_copy(src_ref=src, dst_ref=dst, send_sem=send_sem.at[index],
                                            recv_sem=recv_sem.at[index], device_id=device, device_id_type=MESH)

    def base_of(phase, part, chunk=0):
        return ((phase * CHUNKS + chunk) * PARTS + part) * KINDS

    def local(src, dst, index):
        return pltpu.make_async_copy(src, dst, local_sem.at[index])

    def spread(part, chunk):
        base = base_of(0, part, chunk)
        far, right, left = layer_of(part, 2), layer_of(part, 1), layer_of(part, 3)

        def block(layer, at, size):
            return grad_ref.at[layer, pl.ds(at, size), columns(chunk)]

        def landing(slot, at, size):
            return raw_in(part, slot, chunk).at[pl.ds(at, size)]

        return [
            remote(block(far, 0, half), raw_relay(part, 0, chunk), base + 0, plus[part]),
            remote(block(far, half, half), raw_relay(part, 1, chunk), base + 1, minus[part]),
            remote(block(right, 0, rows), landing(0, 0, rows), base + 2, plus[part]),
            remote(block(left, 0, rows), landing(1, 0, rows), base + 3, minus[part]),
            remote(raw_relay(part, 0, chunk), landing(2, 0, half), base + 4, plus[part]),
            remote(raw_relay(part, 1, chunk), landing(2, half, half), base + 5, minus[part]),
        ]

    def line_block(part, distance, which, chunk):
        at = step_of(axes_of(part)[1], distance) * quarter + which * eighth
        return sum_line(part, chunk).at[pl.ds(pl.multiple_of(at, 8), eighth)]

    def reduce(part, chunk):
        base = base_of(1, part, chunk)
        axis = axes_of(part)[1]

        def landing(slot, which):
            return line_in(part, slot, chunk).at[pl.ds(which * eighth, eighth)]

        return [
            remote(line_block(part, 2, 0, chunk), line_relay(part, 0, chunk), base + 0, plus[axis]),
            remote(line_block(part, 2, 1, chunk), line_relay(part, 1, chunk), base + 1, minus[axis]),
            remote(line_block(part, 1, 1, chunk), landing(0, 1), base + 2, plus[axis]),
            remote(line_block(part, 3, 0, chunk), landing(1, 0), base + 3, minus[axis]),
            remote(line_relay(part, 0, chunk), landing(0, 0), base + 4, plus[axis]),
            remote(line_relay(part, 1, chunk), landing(1, 1), base + 5, minus[axis]),
        ]

    def gather(base, axis, slot):
        here = coord[axis]
        left, right = step_of(axis, 3), step_of(axis, 1)
        return [
            remote(slot(here, 0), slot(here, 0), base + 0, plus[axis]),
            remote(slot(here, 1), slot(here, 1), base + 1, minus[axis]),
            remote(slot(here, 1), slot(here, 1), base + 2, plus[axis]),
            remote(slot(here, 0), slot(here, 0), base + 3, minus[axis]),
            remote(slot(left, 0), slot(left, 0), base + 4, plus[axis]),
            remote(slot(right, 1), slot(right, 1), base + 5, minus[axis]),
        ]

    def launch(copies):
        for copy in copies[:4]:
            copy.start()

    def forward(copies):
        copies[0].wait_recv()
        copies[4].start()
        copies[1].wait_recv()
        copies[5].start()

    def arrive(copies):
        for copy in copies[2:]:
            copy.wait_recv()

    def sent(copies):
        for copy in copies:
            copy.wait_send()

    def over_rows(count, chunk, body):
        def run(index, carry):
            body(pl.ds(pl.multiple_of(index * chunk, chunk), chunk))
            return carry
        lax.fori_loop(0, count // chunk, run, 0)

    fetch_raw, fetch_mom = [], []
    for part in range(PARTS):
        fetch_raw.append(local(grad_ref.at[layer_of(part, 0)], x_buf.at[part // 2, :, pl.ds(part % 2 * cols, cols)], part))
        fetch_mom.append(local(mom_ref.at[layer_of(part, 0)], mom_own(part), PARTS + part))
    for fetch in fetch_raw + fetch_mom:
        fetch.start()

    barrier = pltpu.get_barrier_semaphore()
    for device in plus + minus + [partner]:
        pl.semaphore_signal(barrier, inc=1, device_id=device, device_id_type=MESH)
    pl.semaphore_wait(barrier, 2 * PARTS + 1)

    chunks, parts = range(CHUNKS), range(PARTS)
    copies1 = [[spread(part, chunk) for part in parts] for chunk in chunks]
    copies2 = [[reduce(part, chunk) for part in parts] for chunk in chunks]
    copies3, copies4, copies5, copies6 = ([[] for chunk in chunks] for phase in range(4))

    def sum_raw(part, chunk):
        arrive(copies1[chunk][part])
        own, into = raw_own(part, chunk), sum_line(part, chunk)
        first, second, third = (raw_in(part, slot, chunk) for slot in range(3))

        def add(at):
            total = own[at].astype(jnp.float32) + first[at].astype(jnp.float32)
            into[at] = (total + second[at].astype(jnp.float32)) + third[at].astype(jnp.float32)

        over_rows(rows, 48, add)
        launch(copies2[chunk][part])

    def sum_relay(part, chunk):
        for way, distance in ((0, 1), (1, 3)):
            copies2[chunk][part][way].wait_recv()
            relay, own = line_relay(part, way, chunk), line_block(part, distance, way, chunk)

            def add(at, relay=relay, own=own):
                relay[at] = relay[at] + own[at]

            over_rows(eighth, 24, add)
            copies2[chunk][part][4 + way].start()

    def sum_line_in(part, chunk):
        arrive(copies2[chunk][part])
        axis_c = axes_of(part)[2]
        into = plane(part, coord[axis_c], chunk)
        for which in range(2):
            own = line_block(part, 0, which, chunk)

            def add(at, own=own, which=which):
                row = pl.ds(pl.multiple_of(which * eighth + at.start, 8), at.size)
                into[row] = own[at] + (line_in(part, 0, chunk)[row] + line_in(part, 1, chunk)[row])

            over_rows(eighth, 24, add)

        def slot(index, which):
            return plane(part, index, chunk).at[pl.ds(which * eighth, eighth)]

        copies3[chunk].append(gather(base_of(2, part, chunk), axis_c, slot))
        launch(copies3[chunk][part])

    def sum_plane(part, chunk):
        arrive(copies3[chunk][part])
        axis_b = axes_of(part)[1]
        layer = layer_of(part, 0)
        one, two, three, four = (plane(part, slot, chunk) for slot in range(SIDE))

        def add(at):
            own_at = pl.ds(pl.multiple_of(coord[axis_b] * quarter + at.start, 8), at.size)
            total = (one[at] + two[at]) + (three[at] + four[at])
            mom_out[layer, own_at, columns(chunk)] = total * (1.0 / data_size)

        over_rows(quarter, 48, add)

        def slot(index, which):
            return mom_out.at[layer, pl.ds(pl.multiple_of(index * quarter + which * eighth, 8), eighth), columns(chunk)]

        copies4[chunk].append(gather(base_of(3, part, chunk), axis_b, slot))
        launch(copies4[chunk][part])

    def spread_mean(part, chunk):
        arrive(copies4[chunk][part])

        def slot(index, which):
            return mom_out.at[part * SIDE + index, pl.ds(which * half, half), columns(chunk)]

        copies5[chunk].append(gather(base_of(4, part, chunk), part, slot))
        for copy in copies5[chunk][part][:2]:
            copy.start()

    for part in parts:
        launch(copies1[0][part])
    for part in parts:
        for copy in copies1[1][part][:2]:
            copy.start()
    for part in parts:
        forward(copies1[0][part])
        for copy in copies1[1][part][2:4]:
            copy.start()
    for part in parts:
        forward(copies1[1][part])
    for part in parts:
        fetch_raw[part].wait()
        sum_raw(part, 0)
    for part in parts:
        sum_raw(part, 1)
    for chunk in chunks:
        for part in parts:
            sum_relay(part, chunk)
    for chunk in chunks:
        for part in parts:
            sum_line_in(part, chunk)
    for chunk in chunks:
        for part in parts:
            forward(copies3[chunk][part])
    for chunk in chunks:
        for part in parts:
            sum_plane(part, chunk)
    for chunk in chunks:
        for part in parts:
            forward(copies4[chunk][part])
    for chunk in chunks:
        for part in parts:
            sent(copies1[chunk][part])
            sent(copies2[chunk][part])
            sent(copies3[chunk][part])
    for chunk in chunks:
        for part in parts:
            spread_mean(part, chunk)
    for chunk in chunks:
        for part in parts:
            for copy in copies5[chunk][part][2:4]:
                copy.start()

    swap_base = base_of(PHASES, 0)
    for part in range(PARTS):
        fetch_mom[part].wait()

        def nesterov(at, part=part):
            mean = mom_out[layer_of(part, 0), at]
            nest(part)[at] = mean + MOMENTUM * (MOMENTUM * mom_own(part)[at] + mean)

        over_rows(rows, 16, nesterov)
    give_first = remote(weight_out.at[1 - tp_idx], nest_in.at[0], swap_base, partner)
    give_first.start()
    give_second = remote(nest(2), nest_in.at[1], swap_base + 1, partner)

    @pl.when(tp_idx == 1)
    def _():
        give_second.start()

    weight_base = 2 * PARTS
    fetch_weight = [local(weight_ref.at[layer], weight_out.at[layer], weight_base + layer) for layer in range(layers)]
    for fetch in fetch_weight[PARTS:]:
        fetch.start()

    def orthogonalise(part, which):
        def squares(index, total):
            at = pl.ds(pl.multiple_of(index * 8, 8), 8)
            own, other = weight_out[part, at], nest_in[which, at]
            return total + (own * own + other * other)

        total = lax.fori_loop(0, rows // 8, squares, jnp.zeros((8, cols), jnp.float32))
        scale = 1.0 / (jnp.sqrt(jnp.sum(total, keepdims=True)) + NORM_EPS)

        def normalise(at):
            x_buf[0, at, pl.ds(0, cols)] = (weight_out[part, at] * scale).astype(jnp.bfloat16)
            x_buf[0, at, pl.ds(cols, cols)] = (nest_in[which, at] * scale).astype(jnp.bfloat16)

        over_rows(rows, 16, normalise)

        def newton(step, carry):
            now = lax.rem(step, 2)
            later = 1 - now
            gram_buf[...] = dot_nt(x_buf[now], x_buf[now]).astype(jnp.bfloat16)
            square = dot_nn(gram_buf[...], gram_buf[...])
            poly_buf[...] = (COEF_B * gram_buf[...].astype(jnp.float32) + COEF_C * square).astype(jnp.bfloat16)
            for at in range(0, 2 * cols, cols // 3):
                strip = x_buf[now, :, pl.ds(at, cols // 3)]
                update = dot_nn(poly_buf[...], strip)
                x_buf[later, :, pl.ds(at, cols // 3)] = (COEF_A * strip.astype(jnp.float32) + update).astype(jnp.bfloat16)
            return carry

        lax.fori_loop(0, NS_STEPS, newton, 0)

    final = NS_STEPS % 2
    first_layer = jnp.where(tp_idx == 0, layer_of(0, 0), layer_of(1, 0))

    def keep_half(layer):
        def move(at):
            ortho_all[layer, at] = x_buf[final, at, pl.ds(0, cols)]
        over_rows(rows, 16, move)

    def ortho_gather(part):
        def slot(index, which):
            return ortho_all.at[part * SIDE + index, pl.ds(which * half, half)]

        copies6[0].append(gather(base_of(5, part), part, slot))
        launch(copies6[0][part])

    give_first.wait_recv()
    orthogonalise(tp_idx, 0)
    swap_x = remote(x_buf.at[final, :, pl.ds(cols, cols)], ortho_all.at[first_layer], swap_base + 2, partner)
    swap_x.start()
    for chunk in chunks:
        for part in parts:
            forward(copies5[chunk][part])
    keep_half(first_layer)
    swap_x.wait()
    ortho_gather(0)
    ortho_gather(1)

    give_x = remote(x_buf.at[final, :, pl.ds(cols, cols)], ortho_all.at[layer_of(2, 0)], swap_base + 3, partner)

    @pl.when(tp_idx == 0)
    def _():
        give_second.wait_recv()
        orthogonalise(2, 1)
        give_x.start()
        keep_half(layer_of(2, 0))
        give_x.wait_send()

    @pl.when(tp_idx == 1)
    def _():
        give_x.wait_recv()
        give_second.wait_send()

    ortho_gather(2)
    give_first.wait_send()
    for fetch in fetch_weight[:PARTS]:
        fetch.start()

    stream_base = weight_base + layers
    turns = [(part, distance) for distance in ORDER for part in range(PARTS)]
    fetch_turn = [local(mom_ref.at[layer_of(*turn)], nest_in.at[index % 2], stream_base + index)
                  for index, turn in enumerate(turns)]
    fetch_turn[0].start()
    fetch_turn[1].start()
    for index, (part, distance) in enumerate(turns):
        for chunk in chunks:
            copies = copies5[chunk][part]
            if distance == 0:
                sent(copies4[chunk][part])
                sent(copies[:4])
            elif distance == 3:
                copies[2].wait_recv()
                copies[4].wait_send()
            elif distance == 1:
                copies[3].wait_recv()
                copies[5].wait_send()
            else:
                copies[4].wait_recv()
                copies[5].wait_recv()
        fetch_turn[index].wait()
        layer = layer_of(part, distance)

        def momentum(at, layer=layer, index=index):
            mom_out[layer, at] = MOMENTUM * nest_in[index % 2, at] + mom_out[layer, at]

        over_rows(rows, 16, momentum)
        if index + 2 < len(turns):
            fetch_turn[index + 2].start()

    for part in range(PARTS):
        forward(copies6[0][part])
    for fetch in fetch_weight:
        fetch.wait()
    for part, distance in turns:
        if distance == 3:
            copies6[0][part][2].wait_recv()
        elif distance == 1:
            copies6[0][part][3].wait_recv()
        elif distance == 2:
            copies6[0][part][4].wait_recv()
            copies6[0][part][5].wait_recv()
        layer = layer_of(part, distance)

        def descend(at, layer=layer):
            weight = weight_out[layer, at]
            ortho = ortho_all[layer, at].astype(jnp.float32)
            weight_out[layer, at] = weight - LEARN_RATE * (rms_scale * ortho + WEIGHT_DECAY * weight)

        over_rows(rows, 16, descend)
    for part in range(PARTS):
        sent(copies6[0][part])


def flush(held, mom_ref, weight_ref, sem):
    layers = mom_ref.shape[0]
    copies = []
    for layer in range(layers):
        copies.append(pltpu.make_async_copy(held.at[layer], mom_ref.at[layer], sem.at[layer]))
        copies.append(pltpu.make_async_copy(held.at[layers + layer], weight_ref.at[layer], sem.at[layers + layer]))
    for copy in copies:
        copy.start()
    for copy in copies:
        copy.wait()


def solution(mesh):
    data_size = mesh.shape["data"]
    tp_size = mesh.shape["tp"]
    state_spec = P("stage", None, "tp")
    grad_spec = P("stage", "data", None, "tp")

    def per_device(weight, momentum, grad):
        layers, rows, cols = weight.shape
        copies = PHASES * CHUNKS * PARTS * KINDS + SWAPS
        rms_scale = 0.2 * math.sqrt(max(rows, cols * tp_size))
        bf16, f32 = jnp.bfloat16, jnp.float32
        in_hbm = pl.BlockSpec(memory_space=pltpu.HBM)
        in_vmem = pl.BlockSpec(memory_space=pltpu.VMEM)
        held = pl.pallas_call(
            functools.partial(kernel, rows, cols, data_size, rms_scale),
            out_shape=pltpu.VMEM((2 * layers, rows, cols), f32),
            in_specs=[in_hbm] * 3,
            out_specs=in_vmem,
            scratch_shapes=[
                pltpu.VMEM((layers, rows, cols), bf16),
                pltpu.VMEM((2, rows, tp_size * cols), bf16),
                pltpu.VMEM((rows, rows), bf16),
                pltpu.VMEM((rows, rows), bf16),
                pltpu.VMEM((2, rows, cols), f32),
                pltpu.SemaphoreType.DMA((copies,)),
                pltpu.SemaphoreType.DMA((copies,)),
                pltpu.SemaphoreType.DMA((2 * PARTS + 2 * layers,)),
            ],
            compiler_params=pltpu.CompilerParams(collective_id=0, has_side_effects=True, vmem_limit_bytes=VMEM_KERNEL),
        )(grad.reshape(layers, rows, cols), momentum, weight)
        new_mom, new_weight = pl.pallas_call(
            flush,
            out_shape=(jax.ShapeDtypeStruct((layers, rows, cols), f32),) * 2,
            in_specs=[in_vmem],
            out_specs=(in_hbm,) * 2,
            scratch_shapes=[pltpu.SemaphoreType.DMA((2 * layers,))],
            compiler_params=pltpu.CompilerParams(vmem_limit_bytes=VMEM_FLUSH),
        )(held)
        return new_weight, new_mom

    return jax.shard_map(per_device, mesh=mesh, in_specs=(state_spec, state_spec, grad_spec), out_specs=(state_spec, state_spec), check_vma=False)
```

```python
import functools
import math
import jax
import jax.numpy as jnp
from jax import lax
from jax.experimental import pallas as pl
from jax.experimental.pallas import tpu as pltpu
from jax.sharding import PartitionSpec as P

MOMENTUM = 0.95
LEARN_RATE = 0.25
WEIGHT_DECAY = 0.1
COEF_A = 3.4445
COEF_B = -4.7750
COEF_C = 2.0315
NORM_EPS = 1e-7
NS_STEPS = 5

MESH = pl.DeviceIdType.MESH
SIDE = 4
PARTS = 3
STRIDES = (1, 4, 16)
JOINED = 4
KINDS = 6
CHUNKS = 2
SWAPS = 4
VMEM_KERNEL = 22 * 1024 * 1024
VMEM_FLUSH = 1024 * 1024
ORDER = (0, 3, 1, 2)


def dot_nn(lhs, rhs):
    return lax.dot_general(lhs, rhs, (((1,), (0,)), ((), ())), preferred_element_type=jnp.float32)


def dot_nt(lhs, rhs):
    return lax.dot_general(lhs, rhs, (((1,), (1,)), ((), ())), preferred_element_type=jnp.float32)


def over_rows(count, chunk, body):
    def run(index, carry):
        body(pl.ds(pl.multiple_of(index * chunk, chunk), chunk))
        return carry
    lax.fori_loop(0, count // chunk, run, 0)


def descend(weight_out, ortho_all, rms_scale, layer):
    def add(at):
        weight = weight_out[layer, at]
        ortho = ortho_all[layer, at].astype(jnp.float32)
        weight_out[layer, at] = weight - LEARN_RATE * (rms_scale * ortho + WEIGHT_DECAY * weight)

    over_rows(weight_out.shape[1], 48, add)


def kernel(rows, cols, data_size, rms_scale, grad_ref, mom_ref, weight_ref, held, ortho_all, x_buf, gram_buf, poly_buf,
           nest_in, send_sem, recv_sem, local_sem):
    data_idx = lax.axis_index("data")
    tp_idx = lax.axis_index("tp")
    partner = {"tp": 1 - tp_idx}
    half = rows // 2
    quarter = rows // SIDE
    eighth = quarter // 2
    layers = PARTS * SIDE
    mom_out = held.at[pl.ds(0, layers)]
    weight_out = held.at[pl.ds(layers, layers)]

    width = cols // CHUNKS

    def columns(chunk, start=0):
        return pl.ds(start + chunk * width, width)

    def raw_in(part, slot, chunk):
        return ortho_all.at[part * 3 + slot, :, columns(chunk)]

    def raw_relay(part, way, chunk):
        return ortho_all.at[3 * PARTS + part, pl.ds(way * half, half), columns(chunk)]

    def raw_own(part, chunk):
        return x_buf.at[part // 2, :, columns(chunk, part % 2 * cols)]

    def sum_line(part, chunk):
        return weight_out.at[part, :, columns(chunk)]

    def line_in(part, slot, chunk):
        return weight_out.at[PARTS + part, pl.ds(slot * quarter, quarter), columns(chunk)]

    def line_relay(part, way, chunk):
        return weight_out.at[PARTS + part, pl.ds(2 * quarter + way * eighth, eighth), columns(chunk)]

    def plane(part, slot, chunk):
        return weight_out.at[2 * PARTS + part, pl.ds(pl.multiple_of(slot * quarter, 8), quarter), columns(chunk)]

    def mom_own(part):
        return weight_out.at[3 * PARTS + part]

    def nest(part):
        return weight_out.at[part]

    coord, plus, minus = [], [], []
    for stride in STRIDES:
        here = lax.rem(lax.div(data_idx, stride), SIDE)
        coord.append(here)
        plus.append({"data": data_idx + (lax.rem(here + 1, SIDE) - here) * stride})
        minus.append({"data": data_idx + (lax.rem(here + SIDE - 1, SIDE) - here) * stride})

    def step_of(axis, distance):
        return lax.rem(coord[axis] + distance, SIDE)

    def layer_of(part, distance):
        return part * SIDE + step_of(part, distance)

    def axes_of(part):
        return part, (part + 1) % PARTS, (part + 2) % PARTS

    def remote(src, dst, send, receive, device):
        return pltpu.make_async_remote_copy(src_ref=src, dst_ref=dst, send_sem=send_sem.at[send],
                                            recv_sem=recv_sem.at[receive], device_id=device, device_id_type=MESH)

    def numbers(phase, part, chunk, kind):
        group = chunk * PARTS + part
        send = (phase % 2 * CHUNKS * PARTS + group) * KINDS + kind
        if phase < JOINED:
            return send, (phase * CHUNKS * PARTS + group) * 3 + min(kind, 2)
        return send, (JOINED * 3 + (phase - JOINED) * KINDS) * CHUNKS * PARTS + group * KINDS + kind

    def arrive(phase, part, chunk, landed):
        remote(landed, landed, *numbers(phase, part, chunk, 2), partner).wait_recv()

    def local(src, dst, index):
        return pltpu.make_async_copy(src, dst, local_sem.at[index])

    def spread(part, chunk):
        at_of = functools.partial(numbers, 0, part, chunk)
        far, right, left = layer_of(part, 2), layer_of(part, 1), layer_of(part, 3)

        def block(layer, at, size):
            return grad_ref.at[layer, pl.ds(at, size), columns(chunk)]

        def landing(slot, at, size):
            return raw_in(part, slot, chunk).at[pl.ds(at, size)]

        return [
            remote(block(far, 0, half), raw_relay(part, 0, chunk), *at_of(0), plus[part]),
            remote(block(far, half, half), raw_relay(part, 1, chunk), *at_of(1), minus[part]),
            remote(block(right, 0, rows), landing(0, 0, rows), *at_of(2), plus[part]),
            remote(block(left, 0, rows), landing(1, 0, rows), *at_of(3), minus[part]),
            remote(raw_relay(part, 0, chunk), landing(2, 0, half), *at_of(4), plus[part]),
            remote(raw_relay(part, 1, chunk), landing(2, half, half), *at_of(5), minus[part]),
        ]

    def line_block(part, distance, which, chunk):
        at = step_of(axes_of(part)[1], distance) * quarter + which * eighth
        return sum_line(part, chunk).at[pl.ds(pl.multiple_of(at, 8), eighth)]

    def reduce(part, chunk):
        at_of = functools.partial(numbers, 1, part, chunk)
        axis = axes_of(part)[1]

        def landing(slot, which):
            return line_in(part, slot, chunk).at[pl.ds(which * eighth, eighth)]

        return [
            remote(line_block(part, 2, 0, chunk), line_relay(part, 0, chunk), *at_of(0), plus[axis]),
            remote(line_block(part, 2, 1, chunk), line_relay(part, 1, chunk), *at_of(1), minus[axis]),
            remote(line_block(part, 1, 1, chunk), landing(0, 1), *at_of(2), plus[axis]),
            remote(line_block(part, 3, 0, chunk), landing(1, 0), *at_of(3), minus[axis]),
            remote(line_relay(part, 0, chunk), landing(0, 0), *at_of(4), plus[axis]),
            remote(line_relay(part, 1, chunk), landing(1, 1), *at_of(5), minus[axis]),
        ]

    def gather(phase, part, chunk, axis, slot):
        at_of = functools.partial(numbers, phase, part, chunk)
        here = coord[axis]
        left, right = step_of(axis, 3), step_of(axis, 1)
        return [
            remote(slot(here, 0), slot(here, 0), *at_of(0), plus[axis]),
            remote(slot(here, 1), slot(here, 1), *at_of(1), minus[axis]),
            remote(slot(here, 1), slot(here, 1), *at_of(2), plus[axis]),
            remote(slot(here, 0), slot(here, 0), *at_of(3), minus[axis]),
            remote(slot(left, 0), slot(left, 0), *at_of(4), plus[axis]),
            remote(slot(right, 1), slot(right, 1), *at_of(5), minus[axis]),
        ]

    def launch(copies):
        for copy in copies[:4]:
            copy.start()

    def forward(copies):
        copies[0].wait_recv()
        copies[4].start()
        copies[1].wait_recv()
        copies[5].start()

    def sent(copies):
        for copy in copies:
            copy.wait_send()

    fetch_raw, fetch_mom = [], []
    for part in range(PARTS):
        fetch_raw.append(local(grad_ref.at[layer_of(part, 0)], x_buf.at[part // 2, :, pl.ds(part % 2 * cols, cols)], part))
        fetch_mom.append(local(mom_ref.at[layer_of(part, 0)], mom_own(part), PARTS + part))
    for fetch in fetch_raw + fetch_mom:
        fetch.start()

    barrier = pltpu.get_barrier_semaphore()
    for device in plus + minus + [partner]:
        pl.semaphore_signal(barrier, inc=1, device_id=device, device_id_type=MESH)
    pl.semaphore_wait(barrier, 2 * PARTS + 1)

    chunks, parts = range(CHUNKS), range(PARTS)
    copies1 = [[spread(part, chunk) for part in parts] for chunk in chunks]
    copies2 = [[reduce(part, chunk) for part in parts] for chunk in chunks]
    copies3, copies4, copies5, copies6 = ([[] for chunk in chunks] for phase in range(4))

    def sum_raw(part, chunk):
        arrive(0, part, chunk, ortho_all.at[pl.ds(part * 3, 3), :, columns(chunk)])
        own, into = raw_own(part, chunk), sum_line(part, chunk)
        first, second, third = (raw_in(part, slot, chunk) for slot in range(3))

        def add(at):
            total = own[at].astype(jnp.float32) + first[at].astype(jnp.float32)
            into[at] = (total + second[at].astype(jnp.float32)) + third[at].astype(jnp.float32)

        over_rows(rows, 48, add)
        launch(copies2[chunk][part])

    def sum_relay(part, chunk):
        for way, distance in ((0, 1), (1, 3)):
            copies2[chunk][part][way].wait_recv()
            relay, own = line_relay(part, way, chunk), line_block(part, distance, way, chunk)

            def add(at, relay=relay, own=own):
                relay[at] = relay[at] + own[at]

            over_rows(eighth, 24, add)
            copies2[chunk][part][4 + way].start()

    def sum_line_in(part, chunk):
        arrive(1, part, chunk, weight_out.at[PARTS + part, pl.ds(0, 2 * quarter), columns(chunk)])
        axis_c = axes_of(part)[2]
        into = plane(part, coord[axis_c], chunk)
        for which in range(2):
            own = line_block(part, 0, which, chunk)

            def add(at, own=own, which=which):
                row = pl.ds(pl.multiple_of(which * eighth + at.start, 8), at.size)
                into[row] = own[at] + (line_in(part, 0, chunk)[row] + line_in(part, 1, chunk)[row])

            over_rows(eighth, 24, add)

        def slot(index, which):
            return plane(part, index, chunk).at[pl.ds(which * eighth, eighth)]

        copies3[chunk].append(gather(2, part, chunk, axis_c, slot))
        launch(copies3[chunk][part])

    def sum_plane(part, chunk):
        arrive(2, part, chunk, weight_out.at[2 * PARTS + part, pl.ds(0, 2 * quarter), columns(chunk)])
        axis_b = axes_of(part)[1]
        layer = layer_of(part, 0)
        one, two, three, four = (plane(part, slot, chunk) for slot in range(SIDE))

        def add(at):
            own_at = pl.ds(pl.multiple_of(coord[axis_b] * quarter + at.start, 8), at.size)
            total = (one[at] + two[at]) + (three[at] + four[at])
            mom_out[layer, own_at, columns(chunk)] = total * (1.0 / data_size)

        over_rows(quarter, 48, add)

        def slot(index, which):
            return mom_out.at[layer, pl.ds(pl.multiple_of(index * quarter + which * eighth, 8), eighth), columns(chunk)]

        copies4[chunk].append(gather(3, part, chunk, axis_b, slot))
        launch(copies4[chunk][part])

    def spread_mean(part, chunk):
        arrive(3, part, chunk, mom_out.at[layer_of(part, 0), pl.ds(0, 2 * quarter), columns(chunk)])

        def slot(index, which):
            return mom_out.at[part * SIDE + index, pl.ds(which * half, half), columns(chunk)]

        copies5[chunk].append(gather(4, part, chunk, part, slot))
        for copy in copies5[chunk][part][:2]:
            copy.start()

    for part in parts:
        launch(copies1[0][part])
    for part in parts:
        for copy in copies1[1][part][:2]:
            copy.start()
    for part in parts:
        forward(copies1[0][part])
        for copy in copies1[1][part][2:4]:
            copy.start()
    for part in parts:
        forward(copies1[1][part])
    for part in parts:
        fetch_raw[part].wait()
        sum_raw(part, 0)
    for part in parts:
        sum_raw(part, 1)
    for chunk in chunks:
        for part in parts:
            sum_relay(part, chunk)
    for chunk in chunks:
        for part in parts:
            sent(copies1[chunk][part])
    for chunk in chunks:
        for part in parts:
            sum_line_in(part, chunk)
    for chunk in chunks:
        for part in parts:
            forward(copies3[chunk][part])
    for chunk in chunks:
        for part in parts:
            sent(copies2[chunk][part])
    for chunk in chunks:
        for part in parts:
            sum_plane(part, chunk)
    for chunk in chunks:
        for part in parts:
            forward(copies4[chunk][part])
    for chunk in chunks:
        for part in parts:
            sent(copies3[chunk][part])
    for chunk in chunks:
        for part in parts:
            spread_mean(part, chunk)
    for chunk in chunks:
        for part in parts:
            for copy in copies5[chunk][part][2:4]:
                copy.start()

    swap_send, swap_receive = 2 * CHUNKS * PARTS * KINDS, (JOINED * 3 + KINDS) * CHUNKS * PARTS + KINDS * PARTS
    for part in range(PARTS):
        fetch_mom[part].wait()

        def nesterov(at, part=part):
            mean = mom_out[layer_of(part, 0), at]
            nest(part)[at] = mean + MOMENTUM * (MOMENTUM * mom_own(part)[at] + mean)

        over_rows(rows, 16, nesterov)
    give_first = remote(weight_out.at[1 - tp_idx], nest_in.at[0], swap_send + 0, swap_receive + 0, partner)
    give_first.start()
    give_second = remote(nest(2), nest_in.at[1], swap_send + 1, swap_receive + 1, partner)

    @pl.when(tp_idx == 1)
    def _():
        give_second.start()

    weight_base = 2 * PARTS
    fetch_weight = [local(weight_ref.at[layer], weight_out.at[layer], weight_base) for layer in range(layers)]
    for fetch in fetch_weight[PARTS:]:
        fetch.start()

    def orthogonalise(part, which):
        def squares(index, total):
            at = pl.ds(pl.multiple_of(index * 8, 8), 8)
            own, other = weight_out[part, at], nest_in[which, at]
            return total + (own * own + other * other)

        total = lax.fori_loop(0, rows // 8, squares, jnp.zeros((8, cols), jnp.float32))
        scale = 1.0 / (jnp.sqrt(jnp.sum(total, keepdims=True)) + NORM_EPS)

        def normalise(at):
            x_buf[0, at, pl.ds(0, cols)] = (weight_out[part, at] * scale).astype(jnp.bfloat16)
            x_buf[0, at, pl.ds(cols, cols)] = (nest_in[which, at] * scale).astype(jnp.bfloat16)

        over_rows(rows, 16, normalise)

        def newton(step, carry):
            now = lax.rem(step, 2)
            later = 1 - now
            gram_buf[...] = dot_nt(x_buf[now], x_buf[now]).astype(jnp.bfloat16)
            square = dot_nn(gram_buf[...], gram_buf[...])
            poly_buf[...] = (COEF_B * gram_buf[...].astype(jnp.float32) + COEF_C * square).astype(jnp.bfloat16)
            for at in range(0, 2 * cols, cols // 3):
                strip = x_buf[now, :, pl.ds(at, cols // 3)]
                update = dot_nn(poly_buf[...], strip)
                x_buf[later, :, pl.ds(at, cols // 3)] = (COEF_A * strip.astype(jnp.float32) + update).astype(jnp.bfloat16)
            return carry

        lax.fori_loop(0, NS_STEPS, newton, 0)

    final = NS_STEPS % 2
    first_layer = jnp.where(tp_idx == 0, layer_of(0, 0), layer_of(1, 0))

    def keep_half(layer):
        def move(at):
            ortho_all[layer, at] = x_buf[final, at, pl.ds(0, cols)]
        over_rows(rows, 16, move)

    def ortho_gather(part):
        def slot(index, which):
            return ortho_all.at[part * SIDE + index, pl.ds(which * half, half)]

        copies6[0].append(gather(5, part, 0, part, slot))
        launch(copies6[0][part])

    give_first.wait_recv()
    orthogonalise(tp_idx, 0)
    swap_x = remote(x_buf.at[final, :, pl.ds(cols, cols)], ortho_all.at[first_layer], swap_send + 2, swap_receive + 2, partner)
    swap_x.start()
    for chunk in chunks:
        for part in parts:
            forward(copies5[chunk][part])
    keep_half(first_layer)
    swap_x.wait()
    for chunk in chunks:
        for part in parts:
            sent(copies4[chunk][part])
    ortho_gather(0)
    ortho_gather(1)

    give_x = remote(x_buf.at[final, :, pl.ds(cols, cols)], ortho_all.at[layer_of(2, 0)], swap_send + 3, swap_receive + 3, partner)

    @pl.when(tp_idx == 0)
    def _():
        give_second.wait_recv()
        orthogonalise(2, 1)
        give_x.start()
        keep_half(layer_of(2, 0))
        give_x.wait_send()

    @pl.when(tp_idx == 1)
    def _():
        give_x.wait_recv()
        give_second.wait_send()

    ortho_gather(2)
    give_first.wait_send()
    for fetch in fetch_weight[:PARTS]:
        fetch.start()

    stream_base = weight_base + 1
    turns = [(part, distance) for distance in ORDER for part in range(PARTS)]
    fetch_turn = [local(mom_ref.at[layer_of(*turn)], nest_in.at[index % 2], stream_base + index % 2)
                  for index, turn in enumerate(turns)]
    fetch_turn[0].start()
    fetch_turn[1].start()
    for index, (part, distance) in enumerate(turns):
        for chunk in chunks:
            copies = copies5[chunk][part]
            if distance == 0:
                sent(copies[:4])
            elif distance == 3:
                copies[2].wait_recv()
                copies[4].wait_send()
            elif distance == 1:
                copies[3].wait_recv()
                copies[5].wait_send()
            else:
                copies[4].wait_recv()
                copies[5].wait_recv()
        fetch_turn[index].wait()
        layer = layer_of(part, distance)

        def momentum(at, layer=layer, index=index):
            mom_out[layer, at] = MOMENTUM * nest_in[index % 2, at] + mom_out[layer, at]

        over_rows(rows, 16, momentum)
        if index + 2 < len(turns):
            fetch_turn[index + 2].start()

    for part in range(PARTS):
        forward(copies6[0][part])
    local(weight_ref, weight_out, weight_base).wait()
    for part, distance in turns:
        if distance == 3:
            copies6[0][part][2].wait_recv()
        elif distance == 1:
            copies6[0][part][3].wait_recv()
        elif distance == 2:
            copies6[0][part][4].wait_recv()
            copies6[0][part][5].wait_recv()
        descend(weight_out, ortho_all, rms_scale, layer_of(part, distance))
    for part in parts:
        sent(copies6[0][part])


def flush(held, mom_ref, weight_ref, sem):
    layers = mom_ref.shape[0]
    mom_out = held.at[pl.ds(0, layers)]
    weight_out = held.at[pl.ds(layers, layers)]
    for layer in range(layers):
        pltpu.make_async_copy(mom_out.at[layer], mom_ref.at[layer], sem.at[0]).start()
        pltpu.make_async_copy(weight_out.at[layer], weight_ref.at[layer], sem.at[1]).start()
    pltpu.make_async_copy(mom_out, mom_ref, sem.at[0]).wait()
    pltpu.make_async_copy(weight_out, weight_ref, sem.at[1]).wait()


def solution(mesh):
    data_size = mesh.shape["data"]
    tp_size = mesh.shape["tp"]
    state_spec = P("stage", None, "tp")
    grad_spec = P("stage", "data", None, "tp")

    def per_device(weight, momentum, grad):
        layers, rows, cols = weight.shape
        sends = 2 * CHUNKS * PARTS * KINDS + SWAPS
        receives = (JOINED * 3 + KINDS) * CHUNKS * PARTS + KINDS * PARTS + SWAPS
        rms_scale = 0.2 * math.sqrt(max(rows, cols * tp_size))
        bf16, f32 = jnp.bfloat16, jnp.float32
        in_hbm = pl.BlockSpec(memory_space=pltpu.HBM)
        in_vmem = pl.BlockSpec(memory_space=pltpu.VMEM)
        held = pl.pallas_call(
            functools.partial(kernel, rows, cols, data_size, rms_scale),
            out_shape=pltpu.VMEM((2 * layers, rows, cols), f32),
            in_specs=[in_hbm] * 3,
            out_specs=in_vmem,
            scratch_shapes=[
                pltpu.VMEM((layers, rows, cols), bf16),
                pltpu.VMEM((2, rows, tp_size * cols), bf16),
                pltpu.VMEM((rows, rows), bf16),
                pltpu.VMEM((rows, rows), bf16),
                pltpu.VMEM((2, rows, cols), f32),
                pltpu.SemaphoreType.DMA((sends,)),
                pltpu.SemaphoreType.DMA((receives,)),
                pltpu.SemaphoreType.DMA((2 * PARTS + 3,)),
            ],
            compiler_params=pltpu.CompilerParams(collective_id=0, has_side_effects=True, vmem_limit_bytes=VMEM_KERNEL),
        )(grad.reshape(layers, rows, cols), momentum, weight)
        new_mom, new_weight = pl.pallas_call(
            flush,
            out_shape=(jax.ShapeDtypeStruct((layers, rows, cols), f32),) * 2,
            in_specs=[in_vmem],
            out_specs=(in_hbm,) * 2,
            scratch_shapes=[pltpu.SemaphoreType.DMA((2,))],
            compiler_params=pltpu.CompilerParams(vmem_limit_bytes=VMEM_FLUSH),
        )(held)
        return new_weight, new_mom

    return jax.shard_map(per_device, mesh=mesh, in_specs=(state_spec, state_spec, grad_spec), out_specs=(state_spec, state_spec), check_vma=False)
```

```python
import functools
import math
import jax
import jax.numpy as jnp
from jax import lax
from jax.experimental import pallas as pl
from jax.experimental.pallas import tpu as pltpu
from jax.sharding import PartitionSpec as P

MOMENTUM = 0.95
LEARN_RATE = 0.25
WEIGHT_DECAY = 0.1
COEF_A = 3.4445
COEF_B = -4.7750
COEF_C = 2.0315
NORM_EPS = 1e-7
NS_STEPS = 5

MESH = pl.DeviceIdType.MESH
SIDE = 4
PARTS = 3
STRIDES = (1, 4, 16)
JOINED = 5
KINDS = 6
CHUNKS = 3
GROUPS = (2, 1)
LANES = 128
SPLIT = 40
SWAPS = 4
VMEM_KERNEL = 22 * 1024 * 1024
VMEM_FLUSH = 1024 * 1024
ORDER = (0, 3, 1, 2)


def dot_nn(lhs, rhs):
    return lax.dot_general(lhs, rhs, (((1,), (0,)), ((), ())), preferred_element_type=jnp.float32)


def dot_nt(lhs, rhs):
    return lax.dot_general(lhs, rhs, (((1,), (1,)), ((), ())), preferred_element_type=jnp.float32)


def over_rows(count, chunk, body):
    def run(index, carry):
        body(pl.ds(pl.multiple_of(index * chunk, chunk), chunk))
        return carry
    lax.fori_loop(0, count // chunk, run, 0)


def descend(weight_out, ortho_all, rms_scale, layer):
    def add(at):
        weight = weight_out[layer, at]
        ortho = ortho_all[layer, at].astype(jnp.float32)
        weight_out[layer, at] = weight - LEARN_RATE * (rms_scale * ortho + WEIGHT_DECAY * weight)

    over_rows(weight_out.shape[1], 48, add)


def kernel(rows, cols, data_size, rms_scale, grad_ref, mom_ref, weight_ref, held, ortho_all, x_buf, gram_buf, poly_buf,
           nest_in, send_sem, recv_sem, local_sem):
    data_idx = lax.axis_index("data")
    tp_idx = lax.axis_index("tp")
    partner = {"tp": 1 - tp_idx}
    half = rows // 2
    quarter = rows // SIDE
    eighth = quarter // 2
    layers = PARTS * SIDE
    mom_out = held.at[pl.ds(0, layers)]
    weight_out = held.at[pl.ds(layers, layers)]

    width = cols // CHUNKS

    def columns(chunk, start=0):
        return pl.ds(start + chunk * width, width)

    def raw_in(part, slot, chunk):
        return ortho_all.at[part * 3 + slot, :, columns(chunk)]

    def raw_relay(part, way, chunk):
        return ortho_all.at[3 * PARTS + part, pl.ds(way * half, half), columns(chunk)]

    def raw_own(part, chunk):
        return x_buf.at[part // 2, :, columns(chunk, part % 2 * cols)]

    def sum_line(part, chunk):
        return weight_out.at[part, :, columns(chunk)]

    def line_in(part, slot, chunk):
        return weight_out.at[PARTS + part, pl.ds(slot * quarter, quarter), columns(chunk)]

    def line_relay(part, way, chunk):
        return weight_out.at[PARTS + part, pl.ds(2 * quarter + way * eighth, eighth), columns(chunk)]

    block_rows = eighth

    def block_at(index, which, row, chunk):
        at = row + lax.div(index, 2) * block_rows + which * SPLIT
        size = block_rows - SPLIT if which else SPLIT
        lane = chunk * width + lax.rem(index, 2) * LANES
        return pl.ds(pl.multiple_of(at, 8), size), pl.ds(pl.multiple_of(lane, LANES), LANES)

    def plane(part, chunk):
        return weight_out.at[2 * PARTS + part, pl.ds(0, quarter), columns(chunk)]

    def plane_block(part, index, which, chunk):
        return weight_out.at[2 * PARTS + part, *block_at(index, which, 0, chunk)]

    def plane_in(part, slot, which, chunk):
        size = block_rows - SPLIT if which else SPLIT
        return weight_out.at[2 * PARTS + part, pl.ds(quarter + slot * block_rows + which * SPLIT, size),
                             pl.ds(chunk * width, LANES)]

    def plane_relay(part, way, chunk):
        size = block_rows - SPLIT if way else SPLIT
        return weight_out.at[2 * PARTS + part, pl.ds(quarter + way * SPLIT, size), pl.ds(chunk * width + LANES, LANES)]

    def mom_own(part):
        return weight_out.at[3 * PARTS + part]

    def nest(part):
        return weight_out.at[part]

    coord, plus, minus = [], [], []
    for stride in STRIDES:
        here = lax.rem(lax.div(data_idx, stride), SIDE)
        coord.append(here)
        plus.append({"data": data_idx + (lax.rem(here + 1, SIDE) - here) * stride})
        minus.append({"data": data_idx + (lax.rem(here + SIDE - 1, SIDE) - here) * stride})

    def step_of(axis, distance):
        return lax.rem(coord[axis] + distance, SIDE)

    def layer_of(part, distance):
        return part * SIDE + step_of(part, distance)

    def axes_of(part):
        return part, (part + 1) % PARTS, (part + 2) % PARTS

    def remote(src, dst, send, receive, device):
        return pltpu.make_async_remote_copy(src_ref=src, dst_ref=dst, send_sem=send_sem.at[send],
                                            recv_sem=recv_sem.at[receive], device_id=device, device_id_type=MESH)

    def numbers(phase, part, chunk, kind):
        group = chunk * PARTS + part
        send = phase % 2 * CHUNKS * PARTS + group
        if phase < JOINED:
            return send, (phase * CHUNKS * PARTS + group) * 3 + min(kind, 2)
        later = JOINED * 3 * CHUNKS * PARTS + (phase - JOINED) * len(GROUPS) * PARTS * KINDS
        return send, later + group * KINDS + kind

    def arrive(phase, part, chunk, landed):
        remote(landed, landed, *numbers(phase, part, chunk, 2), partner).wait_recv()

    def sent(phase, part, chunk=0):
        if phase == 0:
            left = ortho_all.at[pl.ds(0, SIDE), :, columns(chunk)]
        elif phase in (1, 4):
            left = weight_out.at[0, pl.ds(0, 3 * quarter), columns(chunk)]
        elif phase in (2, 3):
            left = weight_out.at[0, pl.ds(0, 3 * block_rows), pl.ds(0, LANES)]
        elif phase == 5:
            left = mom_out.at[pl.ds(0, 3), :, group_columns(chunk)]
        else:
            left = ortho_all.at[pl.ds(0, 3)]
        remote(left, left, *numbers(phase, part, chunk, 2), partner).wait_send()

    def group_columns(group):
        return pl.ds(sum(GROUPS[:group]) * width, GROUPS[group] * width)

    def local(src, dst, index):
        return pltpu.make_async_copy(src, dst, local_sem.at[index])

    def spread(part, chunk):
        at_of = functools.partial(numbers, 0, part, chunk)
        far, right, left = layer_of(part, 2), layer_of(part, 1), layer_of(part, 3)

        def block(layer, at, size):
            return grad_ref.at[layer, pl.ds(at, size), columns(chunk)]

        def landing(slot, at, size):
            return raw_in(part, slot, chunk).at[pl.ds(at, size)]

        return [
            remote(block(far, 0, half), raw_relay(part, 0, chunk), *at_of(0), plus[part]),
            remote(block(far, half, half), raw_relay(part, 1, chunk), *at_of(1), minus[part]),
            remote(block(right, 0, rows), landing(0, 0, rows), *at_of(2), plus[part]),
            remote(block(left, 0, rows), landing(1, 0, rows), *at_of(3), minus[part]),
            remote(raw_relay(part, 0, chunk), landing(2, 0, half), *at_of(4), plus[part]),
            remote(raw_relay(part, 1, chunk), landing(2, half, half), *at_of(5), minus[part]),
        ]

    def line_block(part, distance, which, chunk):
        at = step_of(axes_of(part)[1], distance) * quarter + which * eighth
        return sum_line(part, chunk).at[pl.ds(pl.multiple_of(at, 8), eighth)]

    def reduce(phase, part, chunk, axis, block, relay, landing):
        at_of = functools.partial(numbers, phase, part, chunk)
        return [
            remote(block(2, 0), relay(0), *at_of(0), plus[axis]),
            remote(block(2, 1), relay(1), *at_of(1), minus[axis]),
            remote(block(1, 1), landing(0, 1), *at_of(2), plus[axis]),
            remote(block(3, 0), landing(1, 0), *at_of(3), minus[axis]),
            remote(relay(0), landing(0, 0), *at_of(4), plus[axis]),
            remote(relay(1), landing(1, 1), *at_of(5), minus[axis]),
        ]

    def relay_sums(copies, block, relay):
        for way, distance in ((0, 1), (1, 3)):
            copies[way].wait_recv()
            into, own = relay(way), block(distance, way)

            def add(at, into=into, own=own):
                into[at] = into[at] + own[at]

            over_rows(into.shape[0], 8, add)
            copies[4 + way].start()

    def reduce_rows(part, chunk):
        def landing(slot, which):
            return line_in(part, slot, chunk).at[pl.ds(which * eighth, eighth)]

        return reduce(1, part, chunk, axes_of(part)[1], lambda distance, which: line_block(part, distance, which, chunk),
                      lambda way: line_relay(part, way, chunk), landing)

    def third_block(part, distance, which, chunk):
        return plane_block(part, step_of(axes_of(part)[2], distance), which, chunk)

    def reduce_blocks(part, chunk):
        return reduce(2, part, chunk, axes_of(part)[2], lambda distance, which: third_block(part, distance, which, chunk),
                      lambda way: plane_relay(part, way, chunk), lambda slot, which: plane_in(part, slot, which, chunk))

    def gather(phase, part, chunk, axis, slot):
        at_of = functools.partial(numbers, phase, part, chunk)
        here = coord[axis]
        left, right = step_of(axis, 3), step_of(axis, 1)
        return [
            remote(slot(here, 0), slot(here, 0), *at_of(0), plus[axis]),
            remote(slot(here, 1), slot(here, 1), *at_of(1), minus[axis]),
            remote(slot(here, 1), slot(here, 1), *at_of(2), plus[axis]),
            remote(slot(here, 0), slot(here, 0), *at_of(3), minus[axis]),
            remote(slot(left, 0), slot(left, 0), *at_of(4), plus[axis]),
            remote(slot(right, 1), slot(right, 1), *at_of(5), minus[axis]),
        ]

    def launch(copies):
        for copy in copies[:4]:
            copy.start()

    def forward(copies):
        copies[0].wait_recv()
        copies[4].start()
        copies[1].wait_recv()
        copies[5].start()

    fetch_raw, fetch_mom = [], []
    for part in range(PARTS):
        fetch_raw.append(local(grad_ref.at[layer_of(part, 0)], x_buf.at[part // 2, :, pl.ds(part % 2 * cols, cols)], part))
        fetch_mom.append(local(mom_ref.at[layer_of(part, 0)], mom_own(part), PARTS + part))
    for fetch in fetch_raw + fetch_mom:
        fetch.start()

    barrier = pltpu.get_barrier_semaphore()
    for device in plus + minus + [partner]:
        pl.semaphore_signal(barrier, inc=1, device_id=device, device_id_type=MESH)
    pl.semaphore_wait(barrier, 2 * PARTS + 1)

    chunks, parts = range(CHUNKS), range(PARTS)
    copies1 = [[spread(part, chunk) for part in parts] for chunk in chunks]
    copies2 = [[reduce_rows(part, chunk) for part in parts] for chunk in chunks]
    copies3 = [[reduce_blocks(part, chunk) for part in parts] for chunk in chunks]
    copies4, copies5, copies6, copies7 = ({}, {}, {}, {})

    def sum_raw(part, chunk):
        arrive(0, part, chunk, ortho_all.at[pl.ds(part * 3, 3), :, columns(chunk)])
        own, into = raw_own(part, chunk), sum_line(part, chunk)
        first, second, third = (raw_in(part, slot, chunk) for slot in range(3))

        def add(at):
            total = own[at].astype(jnp.float32) + first[at].astype(jnp.float32)
            into[at] = (total + second[at].astype(jnp.float32)) + third[at].astype(jnp.float32)

        over_rows(rows, 48, add)
        launch(copies2[chunk][part])

    def relay_rows(part, chunk):
        relay_sums(copies2[chunk][part], lambda distance, way: line_block(part, distance, way, chunk),
                   lambda way: line_relay(part, way, chunk))

    def sum_rows(part, chunk):
        arrive(1, part, chunk, weight_out.at[PARTS + part, pl.ds(0, 2 * quarter), columns(chunk)])
        into = plane(part, chunk)
        for which in range(2):
            own = line_block(part, 0, which, chunk)

            def add(at, own=own, which=which):
                row = pl.ds(pl.multiple_of(which * eighth + at.start, 8), at.size)
                into[row] = own[at] + (line_in(part, 0, chunk)[row] + line_in(part, 1, chunk)[row])

            over_rows(eighth, 24, add)
        sent(0, part, chunk)
        launch(copies3[chunk][part])

    def relay_blocks(part, chunk):
        relay_sums(copies3[chunk][part], lambda distance, way: third_block(part, distance, way, chunk),
                   lambda way: plane_relay(part, way, chunk))

    def sum_blocks(part, chunk):
        arrive(2, part, chunk, weight_out.at[2 * PARTS + part, pl.ds(0, 2 * block_rows), pl.ds(0, LANES)])
        axis_b, axis_c = axes_of(part)[1:]
        layer = layer_of(part, 0)

        def slot(index, which):
            return mom_out.at[layer, *block_at(index, which, coord[axis_b] * quarter, chunk)]

        for which in range(2):
            into, own = slot(coord[axis_c], which), third_block(part, 0, which, chunk)
            first, second = plane_in(part, 0, which, chunk), plane_in(part, 1, which, chunk)

            def add(at, into=into, own=own, first=first, second=second):
                into[at] = (own[at] + (first[at] + second[at])) * (1.0 / data_size)

            over_rows(own.shape[0], 8, add)
        sent(1, part, chunk)
        copies4[chunk, part] = gather(3, part, chunk, axis_c, slot)
        launch(copies4[chunk, part])

    def gather_rows(part, chunk):
        arrive(3, part, chunk, weight_out.at[0, pl.ds(0, 2 * block_rows), pl.ds(0, LANES)])
        layer = layer_of(part, 0)

        def slot(index, which):
            return mom_out.at[layer, pl.ds(pl.multiple_of(index * quarter + which * eighth, 8), eighth), columns(chunk)]

        sent(2, part, chunk)
        copies5[chunk, part] = gather(4, part, chunk, axes_of(part)[1], slot)
        launch(copies5[chunk, part])

    def gather_means(part, chunk):
        arrive(4, part, chunk, weight_out.at[0, pl.ds(0, 2 * quarter), columns(chunk)])
        ends = [sum(GROUPS[:group + 1]) - 1 for group in range(len(GROUPS))]
        if chunk not in ends:
            return
        group = ends.index(chunk)

        def slot(index, which):
            return mom_out.at[part * SIDE + index, pl.ds(which * half, half), group_columns(group)]

        sent(3, part, group)
        copies6[group, part] = gather(5, part, group, part, slot)
        for copy in copies6[group, part][:2]:
            copy.start()

    for part in parts:
        launch(copies1[0][part])

    def ahead(chunk, kinds):
        if chunk < CHUNKS:
            for part in parts:
                for kind in kinds:
                    copies1[chunk][part][kind].start()

    def forward_raw(part, chunk):
        if part == 0 and chunk == 0:
            ahead(1, (0, 1))
        forward(copies1[chunk][part])
        if part == PARTS - 1:
            ahead(chunk + 1, (2, 3))
            ahead(chunk + 2, (0, 1))

    for part in parts:
        fetch_raw[part].wait()
    stages = [
        forward_raw,
        sum_raw,
        relay_rows,
        sum_rows,
        relay_blocks,
        sum_blocks,
        lambda part, chunk: forward(copies4[chunk, part]),
        gather_rows,
        lambda part, chunk: forward(copies5[chunk, part]),
        gather_means,
    ]
    for tick in range(len(stages) + CHUNKS - 1):
        for chunk in reversed(chunks):
            if 0 <= tick - chunk < len(stages):
                for part in parts:
                    stages[tick - chunk](part, chunk)
    groups = range(len(GROUPS))
    for group in groups:
        for part in parts:
            for copy in copies6[group, part][2:4]:
                copy.start()
    for part in parts:
        for group in range(len(GROUPS), CHUNKS):
            sent(3, part, group)

    swap_send, swap_receive = 2 * CHUNKS * PARTS, JOINED * 3 * CHUNKS * PARTS + (len(GROUPS) + 1) * PARTS * KINDS
    for part in range(PARTS):
        fetch_mom[part].wait()

        def nesterov(at, part=part):
            mean = mom_out[layer_of(part, 0), at]
            nest(part)[at] = mean + MOMENTUM * (MOMENTUM * mom_own(part)[at] + mean)

        over_rows(rows, 16, nesterov)
    give_first = remote(weight_out.at[1 - tp_idx], nest_in.at[0], swap_send + 0, swap_receive + 0, partner)
    give_first.start()
    give_second = remote(nest(2), nest_in.at[1], swap_send + 1, swap_receive + 1, partner)

    @pl.when(tp_idx == 1)
    def _():
        give_second.start()

    weight_base = 2 * PARTS
    fetch_weight = [local(weight_ref.at[layer], weight_out.at[layer], weight_base) for layer in range(layers)]
    for fetch in fetch_weight[PARTS:]:
        fetch.start()

    def orthogonalise(part, which):
        def squares(index, total):
            at = pl.ds(pl.multiple_of(index * 8, 8), 8)
            own, other = weight_out[part, at], nest_in[which, at]
            return total + (own * own + other * other)

        total = lax.fori_loop(0, rows // 8, squares, jnp.zeros((8, cols), jnp.float32))
        scale = 1.0 / (jnp.sqrt(jnp.sum(total, keepdims=True)) + NORM_EPS)

        def normalise(at):
            x_buf[0, at, pl.ds(0, cols)] = (weight_out[part, at] * scale).astype(jnp.bfloat16)
            x_buf[0, at, pl.ds(cols, cols)] = (nest_in[which, at] * scale).astype(jnp.bfloat16)

        over_rows(rows, 16, normalise)

        def newton(step, carry):
            now = lax.rem(step, 2)
            later = 1 - now
            gram_buf[...] = dot_nt(x_buf[now], x_buf[now]).astype(jnp.bfloat16)
            square = dot_nn(gram_buf[...], gram_buf[...])
            poly_buf[...] = (COEF_B * gram_buf[...].astype(jnp.float32) + COEF_C * square).astype(jnp.bfloat16)
            for at in range(0, 2 * cols, cols // 3):
                strip = x_buf[now, :, pl.ds(at, cols // 3)]
                update = dot_nn(poly_buf[...], strip)
                x_buf[later, :, pl.ds(at, cols // 3)] = (COEF_A * strip.astype(jnp.float32) + update).astype(jnp.bfloat16)
            return carry

        lax.fori_loop(0, NS_STEPS, newton, 0)

    final = NS_STEPS % 2
    first_layer = jnp.where(tp_idx == 0, layer_of(0, 0), layer_of(1, 0))

    def keep_half(layer):
        def move(at):
            ortho_all[layer, at] = x_buf[final, at, pl.ds(0, cols)]
        over_rows(rows, 16, move)

    def ortho_gather(part):
        def slot(index, which):
            return ortho_all.at[part * SIDE + index, pl.ds(which * half, half)]

        copies7[part] = gather(6, part, 0, part, slot)
        launch(copies7[part])

    give_first.wait_recv()
    orthogonalise(tp_idx, 0)
    swap_x = remote(x_buf.at[final, :, pl.ds(cols, cols)], ortho_all.at[first_layer], swap_send + 2, swap_receive + 2, partner)
    swap_x.start()
    for group in groups:
        for part in parts:
            forward(copies6[group, part])
    keep_half(first_layer)
    swap_x.wait()
    for chunk in chunks:
        for part in parts:
            sent(4, part, chunk)
    ortho_gather(0)
    ortho_gather(1)

    give_x = remote(x_buf.at[final, :, pl.ds(cols, cols)], ortho_all.at[layer_of(2, 0)], swap_send + 3, swap_receive + 3, partner)

    @pl.when(tp_idx == 0)
    def _():
        give_second.wait_recv()
        orthogonalise(2, 1)
        give_x.start()
        keep_half(layer_of(2, 0))
        give_x.wait_send()

    @pl.when(tp_idx == 1)
    def _():
        give_x.wait_recv()
        give_second.wait_send()

    ortho_gather(2)
    give_first.wait_send()
    for fetch in fetch_weight[:PARTS]:
        fetch.start()

    stream_base = weight_base + 1
    turns = [(part, distance) for distance in ORDER for part in range(PARTS)]
    fetch_turn = [local(mom_ref.at[layer_of(*turn)], nest_in.at[index % 2], stream_base + index % 2)
                  for index, turn in enumerate(turns)]
    fetch_turn[0].start()
    fetch_turn[1].start()
    for index, (part, distance) in enumerate(turns):
        for group in groups:
            if distance == 0:
                sent(5, part, group)
            elif distance == 3:
                copies6[group, part][2].wait_recv()
            elif distance == 1:
                copies6[group, part][3].wait_recv()
            else:
                copies6[group, part][4].wait_recv()
                copies6[group, part][5].wait_recv()
        fetch_turn[index].wait()
        layer = layer_of(part, distance)

        def momentum(at, layer=layer, index=index):
            mom_out[layer, at] = MOMENTUM * nest_in[index % 2, at] + mom_out[layer, at]

        over_rows(rows, 16, momentum)
        if index + 2 < len(turns):
            fetch_turn[index + 2].start()

    for part in range(PARTS):
        forward(copies7[part])
    local(weight_ref, weight_out, weight_base).wait()
    for part, distance in turns:
        if distance == 3:
            copies7[part][2].wait_recv()
        elif distance == 1:
            copies7[part][3].wait_recv()
        elif distance == 2:
            copies7[part][4].wait_recv()
            copies7[part][5].wait_recv()
        descend(weight_out, ortho_all, rms_scale, layer_of(part, distance))
    for part in parts:
        sent(6, part)


def flush(held, mom_ref, weight_ref, sem):
    layers = mom_ref.shape[0]
    mom_out = held.at[pl.ds(0, layers)]
    weight_out = held.at[pl.ds(layers, layers)]
    for layer in range(layers):
        pltpu.make_async_copy(mom_out.at[layer], mom_ref.at[layer], sem.at[0]).start()
        pltpu.make_async_copy(weight_out.at[layer], weight_ref.at[layer], sem.at[1]).start()
    pltpu.make_async_copy(mom_out, mom_ref, sem.at[0]).wait()
    pltpu.make_async_copy(weight_out, weight_ref, sem.at[1]).wait()


def solution(mesh):
    data_size = mesh.shape["data"]
    tp_size = mesh.shape["tp"]
    state_spec = P("stage", None, "tp")
    grad_spec = P("stage", "data", None, "tp")

    def per_device(weight, momentum, grad):
        layers, rows, cols = weight.shape
        sends = 2 * CHUNKS * PARTS + SWAPS
        receives = JOINED * 3 * CHUNKS * PARTS + (len(GROUPS) + 1) * PARTS * KINDS + SWAPS
        rms_scale = 0.2 * math.sqrt(max(rows, cols * tp_size))
        bf16, f32 = jnp.bfloat16, jnp.float32
        in_hbm = pl.BlockSpec(memory_space=pltpu.HBM)
        in_vmem = pl.BlockSpec(memory_space=pltpu.VMEM)
        held = pl.pallas_call(
            functools.partial(kernel, rows, cols, data_size, rms_scale),
            out_shape=pltpu.VMEM((2 * layers, rows, cols), f32),
            in_specs=[in_hbm] * 3,
            out_specs=in_vmem,
            scratch_shapes=[
                pltpu.VMEM((layers, rows, cols), bf16),
                pltpu.VMEM((2, rows, tp_size * cols), bf16),
                pltpu.VMEM((rows, rows), bf16),
                pltpu.VMEM((rows, rows), bf16),
                pltpu.VMEM((2, rows, cols), f32),
                pltpu.SemaphoreType.DMA((sends,)),
                pltpu.SemaphoreType.DMA((receives,)),
                pltpu.SemaphoreType.DMA((2 * PARTS + 3,)),
            ],
            compiler_params=pltpu.CompilerParams(collective_id=0, has_side_effects=True, vmem_limit_bytes=VMEM_KERNEL),
        )(grad.reshape(layers, rows, cols), momentum, weight)
        new_mom, new_weight = pl.pallas_call(
            flush,
            out_shape=(jax.ShapeDtypeStruct((layers, rows, cols), f32),) * 2,
            in_specs=[in_vmem],
            out_specs=(in_hbm,) * 2,
            scratch_shapes=[pltpu.SemaphoreType.DMA((2,))],
            compiler_params=pltpu.CompilerParams(vmem_limit_bytes=VMEM_FLUSH),
        )(held)
        return new_weight, new_mom

    return jax.shard_map(per_device, mesh=mesh, in_specs=(state_spec, state_spec, grad_spec), out_specs=(state_spec, state_spec), check_vma=False)
```

```python
import functools
import math
import jax
import jax.numpy as jnp
from jax import lax
from jax.experimental import pallas as pl
from jax.experimental.pallas import tpu as pltpu
from jax.sharding import PartitionSpec as P

MOMENTUM = 0.95
LEARN_RATE = 0.25
WEIGHT_DECAY = 0.1
COEF_A = 3.4445
COEF_B = -4.7750
COEF_C = 2.0315
NORM_EPS = 1e-7
NS_STEPS = 5

MESH = pl.DeviceIdType.MESH
SIDE = 4
PARTS = 3
STRIDES = (1, 4, 16)
JOINED = 5
LAST_KINDS = 4
KINDS = 6
CHUNKS = 3
GROUPS = (2, 1)
LANES = 128
SPLIT = 40
SWAPS = 4
VMEM_KERNEL = 22 * 1024 * 1024
VMEM_FLUSH = 1024 * 1024
ORDER = (0, 3, 1, 2)


def dot_nn(lhs, rhs):
    return lax.dot_general(lhs, rhs, (((1,), (0,)), ((), ())), preferred_element_type=jnp.float32)


def dot_nt(lhs, rhs):
    return lax.dot_general(lhs, rhs, (((1,), (1,)), ((), ())), preferred_element_type=jnp.float32)


def over_rows(count, chunk, body):
    def run(index, carry):
        body(pl.ds(pl.multiple_of(index * chunk, chunk), chunk))
        return carry
    lax.fori_loop(0, count // chunk, run, 0)


def descend(weight_out, ortho_all, rms_scale, layer):
    def add(at):
        weight = weight_out[layer, at]
        ortho = ortho_all[layer, at].astype(jnp.float32)
        weight_out[layer, at] = weight - LEARN_RATE * (rms_scale * ortho + WEIGHT_DECAY * weight)

    over_rows(weight_out.shape[1], 48, add)


def kernel(rows, cols, data_size, rms_scale, grad_ref, mom_ref, weight_ref, held, ortho_all, x_buf, gram_buf, poly_buf,
           nest_in, send_sem, recv_sem, local_sem):
    data_idx = lax.axis_index("data")
    tp_idx = lax.axis_index("tp")
    partner = {"tp": 1 - tp_idx}
    half = rows // 2
    quarter = rows // SIDE
    eighth = quarter // 2
    layers = PARTS * SIDE
    mom_out = held.at[pl.ds(0, layers)]
    weight_out = held.at[pl.ds(layers, layers)]

    width = cols // CHUNKS

    def columns(chunk, start=0):
        return pl.ds(start + chunk * width, width)

    def raw_in(part, slot, chunk):
        return ortho_all.at[part * 3 + slot, :, columns(chunk)]

    def raw_relay(part, way, chunk):
        return ortho_all.at[3 * PARTS + part, pl.ds(way * half, half), columns(chunk)]

    def raw_own(part, chunk):
        return x_buf.at[part // 2, :, columns(chunk, part % 2 * cols)]

    def sum_line(part, chunk):
        return weight_out.at[part, :, columns(chunk)]

    def line_in(part, slot, chunk):
        return weight_out.at[PARTS + part, pl.ds(slot * quarter, quarter), columns(chunk)]

    def line_relay(part, way, chunk):
        return weight_out.at[PARTS + part, pl.ds(2 * quarter + way * eighth, eighth), columns(chunk)]

    block_rows = eighth

    def block_at(index, which, row, chunk):
        at = row + lax.div(index, 2) * block_rows + which * SPLIT
        size = block_rows - SPLIT if which else SPLIT
        lane = chunk * width + lax.rem(index, 2) * LANES
        return pl.ds(pl.multiple_of(at, 8), size), pl.ds(pl.multiple_of(lane, LANES), LANES)

    def plane(part, chunk):
        return weight_out.at[2 * PARTS + part, pl.ds(0, quarter), columns(chunk)]

    def plane_block(part, index, which, chunk):
        return weight_out.at[2 * PARTS + part, *block_at(index, which, 0, chunk)]

    def plane_in(part, slot, which, chunk):
        size = block_rows - SPLIT if which else SPLIT
        return weight_out.at[2 * PARTS + part, pl.ds(quarter + slot * block_rows + which * SPLIT, size),
                             pl.ds(chunk * width, LANES)]

    def plane_relay(part, way, chunk):
        size = block_rows - SPLIT if way else SPLIT
        return weight_out.at[2 * PARTS + part, pl.ds(quarter + way * SPLIT, size), pl.ds(chunk * width + LANES, LANES)]

    def mom_own(part):
        return weight_out.at[3 * PARTS + part]

    def nest(part):
        return weight_out.at[part]

    coord, plus, minus = [], [], []
    for stride in STRIDES:
        here = lax.rem(lax.div(data_idx, stride), SIDE)
        coord.append(here)
        plus.append({"data": data_idx + (lax.rem(here + 1, SIDE) - here) * stride})
        minus.append({"data": data_idx + (lax.rem(here + SIDE - 1, SIDE) - here) * stride})

    def step_of(axis, distance):
        return lax.rem(coord[axis] + distance, SIDE)

    def layer_of(part, distance):
        return part * SIDE + step_of(part, distance)

    def axes_of(part):
        return part, (part + 1) % PARTS, (part + 2) % PARTS

    def remote(src, dst, send, receive, device):
        return pltpu.make_async_remote_copy(src_ref=src, dst_ref=dst, send_sem=send_sem.at[send],
                                            recv_sem=recv_sem.at[receive], device_id=device, device_id_type=MESH)

    def numbers(phase, part, chunk, kind):
        group = chunk * PARTS + part
        send = phase % 2 * CHUNKS * PARTS + group
        later = JOINED * CHUNKS * PARTS * 2
        if phase < JOINED:
            return send, (phase * CHUNKS * PARTS + group) * 2 + (kind > 1)
        if phase == JOINED:
            return send, later + group * 2 + (kind > 1)
        return send, later + len(GROUPS) * PARTS * 2 + part * LAST_KINDS + (0, 0, 1, 2, 3, 3)[kind]

    def blocks(phase, chunk, count):
        if phase == 0:
            return ortho_all.at[pl.ds(0, count), :, columns(chunk)]
        if phase in (1, 4):
            return weight_out.at[0, pl.ds(0, count * quarter), columns(chunk)]
        if phase in (2, 3):
            return weight_out.at[0, pl.ds(0, count * block_rows), pl.ds(0, LANES)]
        if phase == 5:
            return mom_out.at[pl.ds(0, count), :, group_columns(chunk)]
        return ortho_all.at[pl.ds(0, count)]

    def await_blocks(phase, part, chunk, kind, count):
        landed = blocks(phase, chunk, count)
        remote(landed, landed, *numbers(phase, part, chunk, kind), partner).wait_recv()

    def relayed(phase, part, chunk=0):
        await_blocks(phase, part, chunk, 0, 1)

    def arrive(phase, part, chunk=0):
        await_blocks(phase, part, chunk, 2, 3 if phase == 0 else 2)

    def sent(phase, part, chunk=0):
        left = blocks(phase, chunk, 4 if phase == 0 else 3)
        remote(left, left, *numbers(phase, part, chunk, 2), partner).wait_send()

    def group_columns(group):
        return pl.ds(sum(GROUPS[:group]) * width, GROUPS[group] * width)

    def local(src, dst, index):
        return pltpu.make_async_copy(src, dst, local_sem.at[index])

    def spread(part, chunk):
        at_of = functools.partial(numbers, 0, part, chunk)
        far, right, left = layer_of(part, 2), layer_of(part, 1), layer_of(part, 3)

        def block(layer, at, size):
            return grad_ref.at[layer, pl.ds(at, size), columns(chunk)]

        def landing(slot, at, size):
            return raw_in(part, slot, chunk).at[pl.ds(at, size)]

        return [
            remote(block(far, 0, half), raw_relay(part, 0, chunk), *at_of(0), plus[part]),
            remote(block(far, half, half), raw_relay(part, 1, chunk), *at_of(1), minus[part]),
            remote(block(right, 0, rows), landing(0, 0, rows), *at_of(2), plus[part]),
            remote(block(left, 0, rows), landing(1, 0, rows), *at_of(3), minus[part]),
            remote(raw_relay(part, 0, chunk), landing(2, 0, half), *at_of(4), plus[part]),
            remote(raw_relay(part, 1, chunk), landing(2, half, half), *at_of(5), minus[part]),
        ]

    def line_block(part, distance, which, chunk):
        at = step_of(axes_of(part)[1], distance) * quarter + which * eighth
        return sum_line(part, chunk).at[pl.ds(pl.multiple_of(at, 8), eighth)]

    def reduce(phase, part, chunk, axis, block, relay, landing):
        at_of = functools.partial(numbers, phase, part, chunk)
        return [
            remote(block(2, 0), relay(0), *at_of(0), plus[axis]),
            remote(block(2, 1), relay(1), *at_of(1), minus[axis]),
            remote(block(1, 1), landing(0, 1), *at_of(2), plus[axis]),
            remote(block(3, 0), landing(1, 0), *at_of(3), minus[axis]),
            remote(relay(0), landing(0, 0), *at_of(4), plus[axis]),
            remote(relay(1), landing(1, 1), *at_of(5), minus[axis]),
        ]

    def relay_sums(copies, block, relay):
        for way, distance in ((0, 1), (1, 3)):
            into, own = relay(way), block(distance, way)

            def add(at, into=into, own=own):
                into[at] = into[at] + own[at]

            over_rows(into.shape[0], 8, add)
            copies[4 + way].start()

    def reduce_rows(part, chunk):
        def landing(slot, which):
            return line_in(part, slot, chunk).at[pl.ds(which * eighth, eighth)]

        return reduce(1, part, chunk, axes_of(part)[1], lambda distance, which: line_block(part, distance, which, chunk),
                      lambda way: line_relay(part, way, chunk), landing)

    def third_block(part, distance, which, chunk):
        return plane_block(part, step_of(axes_of(part)[2], distance), which, chunk)

    def reduce_blocks(part, chunk):
        return reduce(2, part, chunk, axes_of(part)[2], lambda distance, which: third_block(part, distance, which, chunk),
                      lambda way: plane_relay(part, way, chunk), lambda slot, which: plane_in(part, slot, which, chunk))

    def gather(phase, part, chunk, axis, slot):
        at_of = functools.partial(numbers, phase, part, chunk)
        here = coord[axis]
        left, right = step_of(axis, 3), step_of(axis, 1)
        return [
            remote(slot(here, 0), slot(here, 0), *at_of(0), plus[axis]),
            remote(slot(here, 1), slot(here, 1), *at_of(1), minus[axis]),
            remote(slot(here, 1), slot(here, 1), *at_of(2), plus[axis]),
            remote(slot(here, 0), slot(here, 0), *at_of(3), minus[axis]),
            remote(slot(left, 0), slot(left, 0), *at_of(4), plus[axis]),
            remote(slot(right, 1), slot(right, 1), *at_of(5), minus[axis]),
        ]

    def launch(copies):
        for copy in copies[:4]:
            copy.start()

    def forward(copies, *where):
        relayed(*where)
        copies[4].start()
        copies[5].start()

    fetch_raw, fetch_mom = [], []
    for part in range(PARTS):
        fetch_raw.append(local(grad_ref.at[layer_of(part, 0)], x_buf.at[part // 2, :, pl.ds(part % 2 * cols, cols)], part))
        fetch_mom.append(local(mom_ref.at[layer_of(part, 0)], mom_own(part), PARTS + part))
    for fetch in fetch_raw + fetch_mom:
        fetch.start()

    barrier = pltpu.get_barrier_semaphore()
    for device in plus + minus + [partner]:
        pl.semaphore_signal(barrier, inc=1, device_id=device, device_id_type=MESH)
    pl.semaphore_wait(barrier, 2 * PARTS + 1)

    chunks, parts = range(CHUNKS), range(PARTS)
    copies1 = [[spread(part, chunk) for part in parts] for chunk in chunks]
    copies2 = [[reduce_rows(part, chunk) for part in parts] for chunk in chunks]
    copies3 = [[reduce_blocks(part, chunk) for part in parts] for chunk in chunks]
    copies4, copies5, copies6, copies7 = ({}, {}, {}, {})

    def sum_raw(part, chunk):
        arrive(0, part, chunk)
        own, into = raw_own(part, chunk), sum_line(part, chunk)
        first, second, third = (raw_in(part, slot, chunk) for slot in range(3))

        def add(at):
            total = own[at].astype(jnp.float32) + first[at].astype(jnp.float32)
            into[at] = (total + second[at].astype(jnp.float32)) + third[at].astype(jnp.float32)

        over_rows(rows, 48, add)
        launch(copies2[chunk][part])

    def relay_rows(part, chunk):
        relayed(1, part, chunk)
        relay_sums(copies2[chunk][part], lambda distance, way: line_block(part, distance, way, chunk),
                   lambda way: line_relay(part, way, chunk))

    def sum_rows(part, chunk):
        arrive(1, part, chunk)
        into = plane(part, chunk)
        for which in range(2):
            own = line_block(part, 0, which, chunk)

            def add(at, own=own, which=which):
                row = pl.ds(pl.multiple_of(which * eighth + at.start, 8), at.size)
                into[row] = own[at] + (line_in(part, 0, chunk)[row] + line_in(part, 1, chunk)[row])

            over_rows(eighth, 24, add)
        sent(0, part, chunk)
        launch(copies3[chunk][part])

    def relay_blocks(part, chunk):
        relayed(2, part, chunk)
        relay_sums(copies3[chunk][part], lambda distance, way: third_block(part, distance, way, chunk),
                   lambda way: plane_relay(part, way, chunk))

    def sum_blocks(part, chunk):
        arrive(2, part, chunk)
        axis_b, axis_c = axes_of(part)[1:]
        layer = layer_of(part, 0)

        def slot(index, which):
            return mom_out.at[layer, *block_at(index, which, coord[axis_b] * quarter, chunk)]

        for which in range(2):
            into, own = slot(coord[axis_c], which), third_block(part, 0, which, chunk)
            first, second = plane_in(part, 0, which, chunk), plane_in(part, 1, which, chunk)

            def add(at, into=into, own=own, first=first, second=second):
                into[at] = (own[at] + (first[at] + second[at])) * (1.0 / data_size)

            over_rows(own.shape[0], 8, add)
        sent(1, part, chunk)
        copies4[chunk, part] = gather(3, part, chunk, axis_c, slot)
        launch(copies4[chunk, part])

    def gather_rows(part, chunk):
        arrive(3, part, chunk)
        layer = layer_of(part, 0)

        def slot(index, which):
            return mom_out.at[layer, pl.ds(pl.multiple_of(index * quarter + which * eighth, 8), eighth), columns(chunk)]

        sent(2, part, chunk)
        copies5[chunk, part] = gather(4, part, chunk, axes_of(part)[1], slot)
        launch(copies5[chunk, part])

    def gather_means(part, chunk):
        arrive(4, part, chunk)
        ends = [sum(GROUPS[:group + 1]) - 1 for group in range(len(GROUPS))]
        if chunk not in ends:
            return
        group = ends.index(chunk)

        def slot(index, which):
            return mom_out.at[part * SIDE + index, pl.ds(which * half, half), group_columns(group)]

        sent(3, part, group)
        copies6[group, part] = gather(5, part, group, part, slot)
        for copy in copies6[group, part][:2]:
            copy.start()

    for part in parts:
        launch(copies1[0][part])

    def ahead(chunk, kinds):
        if chunk < CHUNKS:
            for part in parts:
                for kind in kinds:
                    copies1[chunk][part][kind].start()

    def forward_raw(part, chunk):
        if part == 0 and chunk == 0:
            ahead(1, (0, 1))
        forward(copies1[chunk][part], 0, part, chunk)
        if part == PARTS - 1:
            ahead(chunk + 1, (2, 3))
            ahead(chunk + 2, (0, 1))

    for part in parts:
        fetch_raw[part].wait()
    stages = [
        forward_raw,
        sum_raw,
        relay_rows,
        sum_rows,
        relay_blocks,
        sum_blocks,
        lambda part, chunk: forward(copies4[chunk, part], 3, part, chunk),
        gather_rows,
        lambda part, chunk: forward(copies5[chunk, part], 4, part, chunk),
        gather_means,
    ]
    for tick in range(len(stages) + CHUNKS - 1):
        for chunk in reversed(chunks):
            if 0 <= tick - chunk < len(stages):
                for part in parts:
                    stages[tick - chunk](part, chunk)
    groups = range(len(GROUPS))
    for group in groups:
        for part in parts:
            for copy in copies6[group, part][2:4]:
                copy.start()
    for part in parts:
        for group in range(len(GROUPS), CHUNKS):
            sent(3, part, group)

    swap_send, swap_receive = 2 * CHUNKS * PARTS, JOINED * CHUNKS * PARTS * 2 + PARTS * (len(GROUPS) * 2 + LAST_KINDS)
    for part in range(PARTS):
        fetch_mom[part].wait()

        def nesterov(at, part=part):
            mean = mom_out[layer_of(part, 0), at]
            nest(part)[at] = mean + MOMENTUM * (MOMENTUM * mom_own(part)[at] + mean)

        over_rows(rows, 16, nesterov)
    give_first = remote(weight_out.at[1 - tp_idx], nest_in.at[0], swap_send + 0, swap_receive + 0, partner)
    give_first.start()
    give_second = remote(nest(2), nest_in.at[1], swap_send + 1, swap_receive + 1, partner)

    @pl.when(tp_idx == 1)
    def _():
        give_second.start()

    weight_base = 2 * PARTS
    fetch_weight = [local(weight_ref.at[layer], weight_out.at[layer], weight_base) for layer in range(layers)]
    for fetch in fetch_weight[PARTS:]:
        fetch.start()

    def orthogonalise(part, which, ready=None):
        def squares(index, total):
            at = pl.ds(pl.multiple_of(index * 8, 8), 8)
            own, other = weight_out[part, at], nest_in[which, at]
            return total + (own * own + other * other)

        total = lax.fori_loop(0, rows // 8, squares, jnp.zeros((8, cols), jnp.float32))
        scale = 1.0 / (jnp.sqrt(jnp.sum(total, keepdims=True)) + NORM_EPS)

        def normalise(at):
            x_buf[0, at, pl.ds(0, cols)] = (weight_out[part, at] * scale).astype(jnp.bfloat16)
            x_buf[0, at, pl.ds(cols, cols)] = (nest_in[which, at] * scale).astype(jnp.bfloat16)

        over_rows(rows, 16, normalise)
        if ready is not None:
            ready()

        def newton(step, carry):
            now = lax.rem(step, 2)
            later = 1 - now
            gram_buf[...] = dot_nt(x_buf[now], x_buf[now]).astype(jnp.bfloat16)
            square = dot_nn(gram_buf[...], gram_buf[...])
            poly_buf[...] = (COEF_B * gram_buf[...].astype(jnp.float32) + COEF_C * square).astype(jnp.bfloat16)
            for at in range(0, 2 * cols, cols // 3):
                strip = x_buf[now, :, pl.ds(at, cols // 3)]
                update = dot_nn(poly_buf[...], strip)
                x_buf[later, :, pl.ds(at, cols // 3)] = (COEF_A * strip.astype(jnp.float32) + update).astype(jnp.bfloat16)
            return carry

        lax.fori_loop(0, NS_STEPS, newton, 0)

    final = NS_STEPS % 2
    first_layer = jnp.where(tp_idx == 0, layer_of(0, 0), layer_of(1, 0))

    def keep_half(layer):
        def move(at):
            ortho_all[layer, at] = x_buf[final, at, pl.ds(0, cols)]
        over_rows(rows, 16, move)

    for part in parts:
        def slot(index, which, part=part):
            return ortho_all.at[part * SIDE + index, pl.ds(which * half, half)]

        copies7[part] = gather(6, part, 0, part, slot)

    give_first.wait_recv()
    orthogonalise(tp_idx, 0)
    swap_x = remote(x_buf.at[final, :, pl.ds(cols, cols)], ortho_all.at[first_layer], swap_send + 2, swap_receive + 2, partner)
    swap_x.start()
    for group in groups:
        for part in parts:
            forward(copies6[group, part], 5, part, group)
    keep_half(first_layer)
    for chunk in chunks:
        for part in parts:
            sent(4, part, chunk)
    give_x = remote(x_buf.at[final, :, pl.ds(cols, cols)], ortho_all.at[layer_of(2, 0)], swap_send + 3, swap_receive + 3, partner)

    @pl.when(tp_idx == 0)
    def _():
        launch(copies7[0])
        give_second.wait_recv()
        orthogonalise(2, 1, swap_x.wait_send)
        give_x.start()
        keep_half(layer_of(2, 0))
        launch(copies7[2])
        swap_x.wait_recv()
        launch(copies7[1])
        give_x.wait_send()

    @pl.when(tp_idx == 1)
    def _():
        launch(copies7[1])
        swap_x.wait()
        launch(copies7[0])
        give_x.wait_recv()
        launch(copies7[2])
        give_second.wait_send()

    give_first.wait_send()
    for fetch in fetch_weight[:PARTS]:
        fetch.start()

    stream_base = weight_base + 1
    turns = [(part, distance) for distance in ORDER for part in range(PARTS)]
    fetch_turn = [local(mom_ref.at[layer_of(*turn)], nest_in.at[index % 2], stream_base + index % 2)
                  for index, turn in enumerate(turns)]
    fetch_turn[0].start()
    fetch_turn[1].start()
    for index, (part, distance) in enumerate(turns):
        for group in groups:
            if distance == 0:
                sent(5, part, group)
            elif distance == 3:
                arrive(5, part, group)
        fetch_turn[index].wait()
        layer = layer_of(part, distance)

        def momentum(at, layer=layer, index=index):
            mom_out[layer, at] = MOMENTUM * nest_in[index % 2, at] + mom_out[layer, at]

        over_rows(rows, 16, momentum)
        if index + 2 < len(turns):
            fetch_turn[index + 2].start()

    for part in range(PARTS):
        forward(copies7[part], 6, part)
    local(weight_ref, weight_out, weight_base).wait()
    for part, distance in turns:
        if distance == 3:
            copies7[part][2].wait_recv()
        elif distance == 1:
            copies7[part][3].wait_recv()
        elif distance == 2:
            await_blocks(6, part, 0, 4, 1)
        descend(weight_out, ortho_all, rms_scale, layer_of(part, distance))
    for part in parts:
        sent(6, part)


def flush(held, mom_ref, weight_ref, sem):
    layers = mom_ref.shape[0]
    mom_out = held.at[pl.ds(0, layers)]
    weight_out = held.at[pl.ds(layers, layers)]
    for layer in range(layers):
        pltpu.make_async_copy(mom_out.at[layer], mom_ref.at[layer], sem.at[0]).start()
        pltpu.make_async_copy(weight_out.at[layer], weight_ref.at[layer], sem.at[1]).start()
    pltpu.make_async_copy(mom_out, mom_ref, sem.at[0]).wait()
    pltpu.make_async_copy(weight_out, weight_ref, sem.at[1]).wait()


def solution(mesh):
    data_size = mesh.shape["data"]
    tp_size = mesh.shape["tp"]
    state_spec = P("stage", None, "tp")
    grad_spec = P("stage", "data", None, "tp")

    def per_device(weight, momentum, grad):
        layers, rows, cols = weight.shape
        sends = 2 * CHUNKS * PARTS + SWAPS
        receives = JOINED * CHUNKS * PARTS * 2 + PARTS * (len(GROUPS) * 2 + LAST_KINDS) + SWAPS
        rms_scale = 0.2 * math.sqrt(max(rows, cols * tp_size))
        bf16, f32 = jnp.bfloat16, jnp.float32
        in_hbm = pl.BlockSpec(memory_space=pltpu.HBM)
        in_vmem = pl.BlockSpec(memory_space=pltpu.VMEM)
        held = pl.pallas_call(
            functools.partial(kernel, rows, cols, data_size, rms_scale),
            out_shape=pltpu.VMEM((2 * layers, rows, cols), f32),
            in_specs=[in_hbm] * 3,
            out_specs=in_vmem,
            scratch_shapes=[
                pltpu.VMEM((layers, rows, cols), bf16),
                pltpu.VMEM((2, rows, tp_size * cols), bf16),
                pltpu.VMEM((rows, rows), bf16),
                pltpu.VMEM((rows, rows), bf16),
                pltpu.VMEM((2, rows, cols), f32),
                pltpu.SemaphoreType.DMA((sends,)),
                pltpu.SemaphoreType.DMA((receives,)),
                pltpu.SemaphoreType.DMA((2 * PARTS + 3,)),
            ],
            compiler_params=pltpu.CompilerParams(collective_id=0, has_side_effects=True, vmem_limit_bytes=VMEM_KERNEL),
        )(grad.reshape(layers, rows, cols), momentum, weight)
        new_mom, new_weight = pl.pallas_call(
            flush,
            out_shape=(jax.ShapeDtypeStruct((layers, rows, cols), f32),) * 2,
            in_specs=[in_vmem],
            out_specs=(in_hbm,) * 2,
            scratch_shapes=[pltpu.SemaphoreType.DMA((2,))],
            compiler_params=pltpu.CompilerParams(vmem_limit_bytes=VMEM_FLUSH),
        )(held)
        return new_weight, new_mom

    return jax.shard_map(per_device, mesh=mesh, in_specs=(state_spec, state_spec, grad_spec), out_specs=(state_spec, state_spec), check_vma=False)
```

```python
import functools
import math
import jax
import jax.numpy as jnp
from jax import lax
from jax.experimental import pallas as pl
from jax.experimental.pallas import tpu as pltpu
from jax.sharding import PartitionSpec as P

MOMENTUM = 0.95
LEARN_RATE = 0.25
WEIGHT_DECAY = 0.1
COEF_A = 3.4445
COEF_B = -4.7750
COEF_C = 2.0315
NORM_EPS = 1e-7
NS_STEPS = 5

MESH = pl.DeviceIdType.MESH
SIDE = 4
PARTS = 3
STRIDES = (1, 4, 16)
JOINED = 5
LAST_KINDS = 4
KINDS = 6
CHUNKS = 3
WHOLE = 1
GROUPS = (2, 1)
LANES = 128
SPLIT = 40
SWAPS = 4
VMEM_KERNEL = 22 * 1024 * 1024
VMEM_FLUSH = 1024 * 1024
ORDER = (0, 3, 1, 2)


def dot_nn(lhs, rhs):
    return lax.dot_general(lhs, rhs, (((1,), (0,)), ((), ())), preferred_element_type=jnp.float32)


def dot_nt(lhs, rhs):
    return lax.dot_general(lhs, rhs, (((1,), (1,)), ((), ())), preferred_element_type=jnp.float32)


def over_rows(count, chunk, body):
    def run(index, carry):
        body(pl.ds(pl.multiple_of(index * chunk, chunk), chunk))
        return carry
    lax.fori_loop(0, count // chunk, run, 0)


def descend(weight_out, ortho_all, rms_scale, layer):
    def add(at):
        weight = weight_out[layer, at]
        ortho = ortho_all[layer, at].astype(jnp.float32)
        weight_out[layer, at] = weight - LEARN_RATE * (rms_scale * ortho + WEIGHT_DECAY * weight)

    over_rows(weight_out.shape[1], 48, add)


def kernel(rows, cols, data_size, rms_scale, grad_ref, mom_ref, weight_ref, held, ortho_all, x_buf, gram_buf, poly_buf,
           nest_in, send_sem, recv_sem, local_sem):
    data_idx = lax.axis_index("data")
    tp_idx = lax.axis_index("tp")
    partner = {"tp": 1 - tp_idx}
    half = rows // 2
    quarter = rows // SIDE
    eighth = quarter // 2
    layers = PARTS * SIDE
    mom_out = held.at[pl.ds(0, layers)]
    weight_out = held.at[pl.ds(layers, layers)]

    width = cols // CHUNKS

    def columns(chunk, start=0):
        return pl.ds(start + chunk * width, width)

    def raw_in(part, slot, chunk):
        return ortho_all.at[part * 3 + slot, :, columns(chunk)]

    def raw_relay(part, way, chunk):
        return ortho_all.at[3 * PARTS + part, pl.ds(way * half, half), columns(chunk)]

    def raw_own(part, chunk):
        return x_buf.at[part // 2, :, columns(chunk, part % 2 * cols)]

    def sum_line(part, chunk):
        return weight_out.at[part, :, columns(chunk)]

    def line_in(part, slot, chunk):
        return weight_out.at[PARTS + part, pl.ds(slot * quarter, quarter), columns(chunk)]

    def line_relay(part, way, chunk):
        return weight_out.at[PARTS + part, pl.ds(2 * quarter + way * eighth, eighth), columns(chunk)]

    block_rows = eighth

    def block_at(index, which, row, chunk):
        at = row + lax.div(index, 2) * block_rows + which * SPLIT
        size = block_rows - SPLIT if which else SPLIT
        lane = chunk * width + lax.rem(index, 2) * LANES
        return pl.ds(pl.multiple_of(at, 8), size), pl.ds(pl.multiple_of(lane, LANES), LANES)

    def plane(part, chunk, slot=0):
        at = pl.ds(pl.multiple_of(slot * quarter, 8), quarter)
        return weight_out.at[2 * PARTS + part, at, columns(chunk)]

    def plane_block(part, index, which, chunk):
        return weight_out.at[2 * PARTS + part, *block_at(index, which, 0, chunk)]

    def plane_in(part, slot, which, chunk):
        size = block_rows - SPLIT if which else SPLIT
        return weight_out.at[2 * PARTS + part, pl.ds(quarter + slot * block_rows + which * SPLIT, size),
                             pl.ds(chunk * width, LANES)]

    def plane_relay(part, way, chunk):
        size = block_rows - SPLIT if way else SPLIT
        return weight_out.at[2 * PARTS + part, pl.ds(quarter + way * SPLIT, size), pl.ds(chunk * width + LANES, LANES)]

    def mom_own(part):
        return weight_out.at[3 * PARTS + part]

    def nest(part):
        return weight_out.at[part]

    coord, plus, minus = [], [], []
    for stride in STRIDES:
        here = lax.rem(lax.div(data_idx, stride), SIDE)
        coord.append(here)
        plus.append({"data": data_idx + (lax.rem(here + 1, SIDE) - here) * stride})
        minus.append({"data": data_idx + (lax.rem(here + SIDE - 1, SIDE) - here) * stride})

    def step_of(axis, distance):
        return lax.rem(coord[axis] + distance, SIDE)

    def layer_of(part, distance):
        return part * SIDE + step_of(part, distance)

    def axes_of(part):
        return part, (part + 1) % PARTS, (part + 2) % PARTS

    def remote(src, dst, send, receive, device):
        return pltpu.make_async_remote_copy(src_ref=src, dst_ref=dst, send_sem=send_sem.at[send],
                                            recv_sem=recv_sem.at[receive], device_id=device, device_id_type=MESH)

    def numbers(phase, part, chunk, kind):
        group = chunk * PARTS + part
        send = phase % 2 * CHUNKS * PARTS + group
        later = JOINED * CHUNKS * PARTS * 2
        if phase < JOINED:
            return send, (phase * CHUNKS * PARTS + group) * 2 + (kind > 1)
        if phase == JOINED:
            return send, later + group * 2 + (kind > 1)
        return send, later + len(GROUPS) * PARTS * 2 + part * LAST_KINDS + (0, 0, 1, 2, 3, 3)[kind]

    def blocks(phase, chunk, count):
        if phase == 0:
            return ortho_all.at[pl.ds(0, count), :, columns(chunk)]
        if phase in (1, 4) or (phase == 2 and chunk < WHOLE):
            return weight_out.at[0, pl.ds(0, count * quarter), columns(chunk)]
        if phase in (2, 3):
            return weight_out.at[0, pl.ds(0, count * block_rows), pl.ds(0, LANES)]
        if phase == 5:
            return mom_out.at[pl.ds(0, count), :, group_columns(chunk)]
        return ortho_all.at[pl.ds(0, count)]

    def await_blocks(phase, part, chunk, kind, count):
        landed = blocks(phase, chunk, count)
        remote(landed, landed, *numbers(phase, part, chunk, kind), partner).wait_recv()

    def relayed(phase, part, chunk=0):
        await_blocks(phase, part, chunk, 0, 1)

    def arrive(phase, part, chunk=0):
        await_blocks(phase, part, chunk, 2, 3 if phase == 0 else 2)

    def sent(phase, part, chunk=0):
        left = blocks(phase, chunk, 4 if phase == 0 else 3)
        remote(left, left, *numbers(phase, part, chunk, 2), partner).wait_send()

    def group_columns(group):
        return pl.ds(sum(GROUPS[:group]) * width, GROUPS[group] * width)

    def local(src, dst, index):
        return pltpu.make_async_copy(src, dst, local_sem.at[index])

    def spread(part, chunk):
        at_of = functools.partial(numbers, 0, part, chunk)
        far, right, left = layer_of(part, 2), layer_of(part, 1), layer_of(part, 3)

        def block(layer, at, size):
            return grad_ref.at[layer, pl.ds(at, size), columns(chunk)]

        def landing(slot, at, size):
            return raw_in(part, slot, chunk).at[pl.ds(at, size)]

        return [
            remote(block(far, 0, half), raw_relay(part, 0, chunk), *at_of(0), plus[part]),
            remote(block(far, half, half), raw_relay(part, 1, chunk), *at_of(1), minus[part]),
            remote(block(right, 0, rows), landing(0, 0, rows), *at_of(2), plus[part]),
            remote(block(left, 0, rows), landing(1, 0, rows), *at_of(3), minus[part]),
            remote(raw_relay(part, 0, chunk), landing(2, 0, half), *at_of(4), plus[part]),
            remote(raw_relay(part, 1, chunk), landing(2, half, half), *at_of(5), minus[part]),
        ]

    def line_block(part, distance, which, chunk):
        at = step_of(axes_of(part)[1], distance) * quarter + which * eighth
        return sum_line(part, chunk).at[pl.ds(pl.multiple_of(at, 8), eighth)]

    def reduce(phase, part, chunk, axis, block, relay, landing):
        at_of = functools.partial(numbers, phase, part, chunk)
        return [
            remote(block(2, 0), relay(0), *at_of(0), plus[axis]),
            remote(block(2, 1), relay(1), *at_of(1), minus[axis]),
            remote(block(1, 1), landing(0, 1), *at_of(2), plus[axis]),
            remote(block(3, 0), landing(1, 0), *at_of(3), minus[axis]),
            remote(relay(0), landing(0, 0), *at_of(4), plus[axis]),
            remote(relay(1), landing(1, 1), *at_of(5), minus[axis]),
        ]

    def relay_sums(copies, block, relay):
        for way, distance in ((0, 1), (1, 3)):
            into, own = relay(way), block(distance, way)

            def add(at, into=into, own=own):
                into[at] = into[at] + own[at]

            over_rows(into.shape[0], 8, add)
            copies[4 + way].start()

    def reduce_rows(part, chunk):
        def landing(slot, which):
            return line_in(part, slot, chunk).at[pl.ds(which * eighth, eighth)]

        return reduce(1, part, chunk, axes_of(part)[1], lambda distance, which: line_block(part, distance, which, chunk),
                      lambda way: line_relay(part, way, chunk), landing)

    def third_block(part, distance, which, chunk):
        return plane_block(part, step_of(axes_of(part)[2], distance), which, chunk)

    def reduce_blocks(part, chunk):
        return reduce(2, part, chunk, axes_of(part)[2], lambda distance, which: third_block(part, distance, which, chunk),
                      lambda way: plane_relay(part, way, chunk), lambda slot, which: plane_in(part, slot, which, chunk))

    def gather(phase, part, chunk, axis, slot):
        at_of = functools.partial(numbers, phase, part, chunk)
        here = coord[axis]
        left, right = step_of(axis, 3), step_of(axis, 1)
        return [
            remote(slot(here, 0), slot(here, 0), *at_of(0), plus[axis]),
            remote(slot(here, 1), slot(here, 1), *at_of(1), minus[axis]),
            remote(slot(here, 1), slot(here, 1), *at_of(2), plus[axis]),
            remote(slot(here, 0), slot(here, 0), *at_of(3), minus[axis]),
            remote(slot(left, 0), slot(left, 0), *at_of(4), plus[axis]),
            remote(slot(right, 1), slot(right, 1), *at_of(5), minus[axis]),
        ]

    def launch(copies):
        for copy in copies[:4]:
            copy.start()

    def forward(copies, *where):
        relayed(*where)
        copies[4].start()
        copies[5].start()

    fetch_raw, fetch_mom = [], []
    for part in range(PARTS):
        fetch_raw.append(local(grad_ref.at[layer_of(part, 0)], x_buf.at[part // 2, :, pl.ds(part % 2 * cols, cols)], part))
        fetch_mom.append(local(mom_ref.at[layer_of(part, 0)], mom_own(part), PARTS + part))
    for fetch in fetch_raw + fetch_mom:
        fetch.start()

    barrier = pltpu.get_barrier_semaphore()
    for device in plus + minus + [partner]:
        pl.semaphore_signal(barrier, inc=1, device_id=device, device_id_type=MESH)
    pl.semaphore_wait(barrier, 2 * PARTS + 1)

    chunks, parts = range(CHUNKS), range(PARTS)
    copies1 = [[spread(part, chunk) for part in parts] for chunk in chunks]
    copies2 = [[reduce_rows(part, chunk) for part in parts] for chunk in chunks]

    def exchange(part, chunk):
        def slot(index, which):
            return plane(part, chunk, index).at[pl.ds(which * eighth, eighth)]

        return gather(2, part, chunk, axes_of(part)[2], slot)

    copies3 = [[(exchange if chunk < WHOLE else reduce_blocks)(part, chunk) for part in parts] for chunk in chunks]
    copies4, copies5, copies6, copies7 = ({}, {}, {}, {})

    def sum_raw(part, chunk):
        arrive(0, part, chunk)
        own, into = raw_own(part, chunk), sum_line(part, chunk)
        first, second, third = (raw_in(part, slot, chunk) for slot in range(3))

        def add(at):
            total = own[at].astype(jnp.float32) + first[at].astype(jnp.float32)
            into[at] = (total + second[at].astype(jnp.float32)) + third[at].astype(jnp.float32)

        over_rows(rows, 48, add)
        launch(copies2[chunk][part])

    def relay_rows(part, chunk):
        relayed(1, part, chunk)
        relay_sums(copies2[chunk][part], lambda distance, way: line_block(part, distance, way, chunk),
                   lambda way: line_relay(part, way, chunk))

    def sum_rows(part, chunk):
        arrive(1, part, chunk)
        into = plane(part, chunk, coord[axes_of(part)[2]] if chunk < WHOLE else 0)
        for which in range(2):
            own = line_block(part, 0, which, chunk)

            def add(at, own=own, which=which):
                row = pl.ds(pl.multiple_of(which * eighth + at.start, 8), at.size)
                into[row] = own[at] + (line_in(part, 0, chunk)[row] + line_in(part, 1, chunk)[row])

            over_rows(eighth, 24, add)
        sent(0, part, chunk)
        launch(copies3[chunk][part])

    def relay_blocks(part, chunk):
        relayed(2, part, chunk)
        relay_sums(copies3[chunk][part], lambda distance, way: third_block(part, distance, way, chunk),
                   lambda way: plane_relay(part, way, chunk))

    def sum_blocks(part, chunk):
        arrive(2, part, chunk)
        axis_b, axis_c = axes_of(part)[1:]
        layer = layer_of(part, 0)

        def slot(index, which):
            return mom_out.at[layer, *block_at(index, which, coord[axis_b] * quarter, chunk)]

        for which in range(2):
            into, own = slot(coord[axis_c], which), third_block(part, 0, which, chunk)
            first, second = plane_in(part, 0, which, chunk), plane_in(part, 1, which, chunk)

            def add(at, into=into, own=own, first=first, second=second):
                into[at] = (own[at] + (first[at] + second[at])) * (1.0 / data_size)

            over_rows(own.shape[0], 8, add)
        sent(1, part, chunk)
        copies4[chunk, part] = gather(3, part, chunk, axis_c, slot)
        launch(copies4[chunk, part])

    def sum_planes(part, chunk):
        arrive(2, part, chunk)
        layer, axis_b = layer_of(part, 0), axes_of(part)[1]
        one, two, three, four = (plane(part, chunk, slot) for slot in range(SIDE))
        into = mom_out.at[layer, pl.ds(pl.multiple_of(coord[axis_b] * quarter, 8), quarter), columns(chunk)]

        def add(at):
            into[at] = ((one[at] + two[at]) + (three[at] + four[at])) * (1.0 / data_size)

        over_rows(quarter, 48, add)
        sent(1, part, chunk)
        spread_rows(part, chunk)

    def gather_rows(part, chunk):
        arrive(3, part, chunk)
        spread_rows(part, chunk)

    def spread_rows(part, chunk):
        layer = layer_of(part, 0)

        def slot(index, which):
            return mom_out.at[layer, pl.ds(pl.multiple_of(index * quarter + which * eighth, 8), eighth), columns(chunk)]

        sent(2, part, chunk)
        copies5[chunk, part] = gather(4, part, chunk, axes_of(part)[1], slot)
        launch(copies5[chunk, part])

    def gather_means(part, chunk):
        arrive(4, part, chunk)
        ends = [sum(GROUPS[:group + 1]) - 1 for group in range(len(GROUPS))]
        if chunk not in ends:
            return
        group = ends.index(chunk)

        def slot(index, which):
            return mom_out.at[part * SIDE + index, pl.ds(which * half, half), group_columns(group)]

        if group >= WHOLE:
            sent(3, part, group)
        copies6[group, part] = gather(5, part, group, part, slot)
        for copy in copies6[group, part][:2]:
            copy.start()

    for part in parts:
        launch(copies1[0][part])

    def ahead(chunk, kinds):
        if chunk < CHUNKS:
            for part in parts:
                for kind in kinds:
                    copies1[chunk][part][kind].start()

    def forward_raw(part, chunk):
        if part == 0 and chunk == 0:
            ahead(1, (0, 1))
        forward(copies1[chunk][part], 0, part, chunk)
        if part == PARTS - 1:
            ahead(chunk + 1, (2, 3))
            ahead(chunk + 2, (0, 1))

    for part in parts:
        fetch_raw[part].wait()
    stages = [
        forward_raw,
        sum_raw,
        relay_rows,
        sum_rows,
        relay_blocks,
        sum_blocks,
        lambda part, chunk: forward(copies4[chunk, part], 3, part, chunk),
        gather_rows,
        lambda part, chunk: forward(copies5[chunk, part], 4, part, chunk),
        gather_means,
    ]
    stages_whole = stages[:4] + [
        lambda part, chunk: forward(copies3[chunk][part], 2, part, chunk),
        sum_planes,
        None,
        stages[8],
        None,
        gather_means,
    ]
    for tick in range(len(stages) + CHUNKS - 1):
        for chunk in reversed(chunks):
            if 0 <= tick - chunk < len(stages):
                stage = (stages_whole if chunk < WHOLE else stages)[tick - chunk]
                for part in parts if stage else ():
                    stage(part, chunk)
    groups = range(len(GROUPS))
    for group in groups:
        for part in parts:
            for copy in copies6[group, part][2:4]:
                copy.start()
    for part in parts:
        for group in range(len(GROUPS), CHUNKS):
            sent(3, part, group)

    swap_send, swap_receive = 2 * CHUNKS * PARTS, JOINED * CHUNKS * PARTS * 2 + PARTS * (len(GROUPS) * 2 + LAST_KINDS)
    for part in range(PARTS):
        fetch_mom[part].wait()

        def nesterov(at, part=part):
            mean = mom_out[layer_of(part, 0), at]
            nest(part)[at] = mean + MOMENTUM * (MOMENTUM * mom_own(part)[at] + mean)

        over_rows(rows, 16, nesterov)
    give_first = remote(weight_out.at[1 - tp_idx], nest_in.at[0], swap_send + 0, swap_receive + 0, partner)
    give_first.start()
    give_second = remote(nest(2), nest_in.at[1], swap_send + 1, swap_receive + 1, partner)

    @pl.when(tp_idx == 1)
    def _():
        give_second.start()

    weight_base = 2 * PARTS
    fetch_weight = [local(weight_ref.at[layer], weight_out.at[layer], weight_base) for layer in range(layers)]
    for fetch in fetch_weight[PARTS:]:
        fetch.start()

    def orthogonalise(part, which, ready=None):
        def squares(index, total):
            at = pl.ds(pl.multiple_of(index * 8, 8), 8)
            own, other = weight_out[part, at], nest_in[which, at]
            return total + (own * own + other * other)

        total = lax.fori_loop(0, rows // 8, squares, jnp.zeros((8, cols), jnp.float32))
        scale = 1.0 / (jnp.sqrt(jnp.sum(total, keepdims=True)) + NORM_EPS)

        def normalise(at):
            x_buf[0, at, pl.ds(0, cols)] = (weight_out[part, at] * scale).astype(jnp.bfloat16)
            x_buf[0, at, pl.ds(cols, cols)] = (nest_in[which, at] * scale).astype(jnp.bfloat16)

        over_rows(rows, 16, normalise)
        if ready is not None:
            ready()

        def newton(step, carry):
            now = lax.rem(step, 2)
            later = 1 - now
            gram_buf[...] = dot_nt(x_buf[now], x_buf[now]).astype(jnp.bfloat16)
            square = dot_nn(gram_buf[...], gram_buf[...])
            poly_buf[...] = (COEF_B * gram_buf[...].astype(jnp.float32) + COEF_C * square).astype(jnp.bfloat16)
            for at in range(0, 2 * cols, cols // 3):
                strip = x_buf[now, :, pl.ds(at, cols // 3)]
                update = dot_nn(poly_buf[...], strip)
                x_buf[later, :, pl.ds(at, cols // 3)] = (COEF_A * strip.astype(jnp.float32) + update).astype(jnp.bfloat16)
            return carry

        lax.fori_loop(0, NS_STEPS, newton, 0)

    final = NS_STEPS % 2
    first_layer = jnp.where(tp_idx == 0, layer_of(0, 0), layer_of(1, 0))

    def keep_half(layer):
        def move(at):
            ortho_all[layer, at] = x_buf[final, at, pl.ds(0, cols)]
        over_rows(rows, 16, move)

    for part in parts:
        def slot(index, which, part=part):
            return ortho_all.at[part * SIDE + index, pl.ds(which * half, half)]

        copies7[part] = gather(6, part, 0, part, slot)

    give_first.wait_recv()
    orthogonalise(tp_idx, 0)
    swap_x = remote(x_buf.at[final, :, pl.ds(cols, cols)], ortho_all.at[first_layer], swap_send + 2, swap_receive + 2, partner)
    swap_x.start()
    for group in groups:
        for part in parts:
            forward(copies6[group, part], 5, part, group)
    keep_half(first_layer)
    for chunk in chunks:
        for part in parts:
            sent(4, part, chunk)
    give_x = remote(x_buf.at[final, :, pl.ds(cols, cols)], ortho_all.at[layer_of(2, 0)], swap_send + 3, swap_receive + 3, partner)

    @pl.when(tp_idx == 0)
    def _():
        launch(copies7[0])
        give_second.wait_recv()
        orthogonalise(2, 1, swap_x.wait_send)
        give_x.start()
        keep_half(layer_of(2, 0))
        launch(copies7[2])
        swap_x.wait_recv()
        launch(copies7[1])
        give_x.wait_send()

    @pl.when(tp_idx == 1)
    def _():
        launch(copies7[1])
        swap_x.wait()
        launch(copies7[0])
        give_x.wait_recv()
        launch(copies7[2])
        give_second.wait_send()

    give_first.wait_send()
    for fetch in fetch_weight[:PARTS]:
        fetch.start()

    stream_base = weight_base + 1
    turns = [(part, distance) for distance in ORDER for part in range(PARTS)]
    fetch_turn = [local(mom_ref.at[layer_of(*turn)], nest_in.at[index % 2], stream_base + index % 2)
                  for index, turn in enumerate(turns)]
    fetch_turn[0].start()
    fetch_turn[1].start()
    for index, (part, distance) in enumerate(turns):
        for group in groups:
            if distance == 0:
                sent(5, part, group)
            elif distance == 3:
                arrive(5, part, group)
        fetch_turn[index].wait()
        layer = layer_of(part, distance)

        def momentum(at, layer=layer, index=index):
            mom_out[layer, at] = MOMENTUM * nest_in[index % 2, at] + mom_out[layer, at]

        over_rows(rows, 16, momentum)
        if index + 2 < len(turns):
            fetch_turn[index + 2].start()

    for part in range(PARTS):
        forward(copies7[part], 6, part)
    local(weight_ref, weight_out, weight_base).wait()
    for part, distance in turns:
        if distance == 3:
            copies7[part][2].wait_recv()
        elif distance == 1:
            copies7[part][3].wait_recv()
        elif distance == 2:
            await_blocks(6, part, 0, 4, 1)
        descend(weight_out, ortho_all, rms_scale, layer_of(part, distance))
    for part in parts:
        sent(6, part)


def flush(held, mom_ref, weight_ref, sem):
    layers = mom_ref.shape[0]
    mom_out = held.at[pl.ds(0, layers)]
    weight_out = held.at[pl.ds(layers, layers)]
    for layer in range(layers):
        pltpu.make_async_copy(mom_out.at[layer], mom_ref.at[layer], sem.at[0]).start()
        pltpu.make_async_copy(weight_out.at[layer], weight_ref.at[layer], sem.at[1]).start()
    pltpu.make_async_copy(mom_out, mom_ref, sem.at[0]).wait()
    pltpu.make_async_copy(weight_out, weight_ref, sem.at[1]).wait()


def solution(mesh):
    data_size = mesh.shape["data"]
    tp_size = mesh.shape["tp"]
    state_spec = P("stage", None, "tp")
    grad_spec = P("stage", "data", None, "tp")

    def per_device(weight, momentum, grad):
        layers, rows, cols = weight.shape
        sends = 2 * CHUNKS * PARTS + SWAPS
        receives = JOINED * CHUNKS * PARTS * 2 + PARTS * (len(GROUPS) * 2 + LAST_KINDS) + SWAPS
        rms_scale = 0.2 * math.sqrt(max(rows, cols * tp_size))
        bf16, f32 = jnp.bfloat16, jnp.float32
        in_hbm = pl.BlockSpec(memory_space=pltpu.HBM)
        in_vmem = pl.BlockSpec(memory_space=pltpu.VMEM)
        held = pl.pallas_call(
            functools.partial(kernel, rows, cols, data_size, rms_scale),
            out_shape=pltpu.VMEM((2 * layers, rows, cols), f32),
            in_specs=[in_hbm] * 3,
            out_specs=in_vmem,
            scratch_shapes=[
                pltpu.VMEM((layers, rows, cols), bf16),
                pltpu.VMEM((2, rows, tp_size * cols), bf16),
                pltpu.VMEM((rows, rows), bf16),
                pltpu.VMEM((rows, rows), bf16),
                pltpu.VMEM((2, rows, cols), f32),
                pltpu.SemaphoreType.DMA((sends,)),
                pltpu.SemaphoreType.DMA((receives,)),
                pltpu.SemaphoreType.DMA((2 * PARTS + 3,)),
            ],
            compiler_params=pltpu.CompilerParams(collective_id=0, has_side_effects=True, vmem_limit_bytes=VMEM_KERNEL),
        )(grad.reshape(layers, rows, cols), momentum, weight)
        new_mom, new_weight = pl.pallas_call(
            flush,
            out_shape=(jax.ShapeDtypeStruct((layers, rows, cols), f32),) * 2,
            in_specs=[in_vmem],
            out_specs=(in_hbm,) * 2,
            scratch_shapes=[pltpu.SemaphoreType.DMA((2,))],
            compiler_params=pltpu.CompilerParams(vmem_limit_bytes=VMEM_FLUSH),
        )(held)
        return new_weight, new_mom

    return jax.shard_map(per_device, mesh=mesh, in_specs=(state_spec, state_spec, grad_spec), out_specs=(state_spec, state_spec), check_vma=False)
```

```python
import functools
import math
import jax
import jax.numpy as jnp
from jax import lax
from jax.experimental import pallas as pl
from jax.experimental.pallas import tpu as pltpu
from jax.sharding import PartitionSpec as P

MOMENTUM = 0.95
LEARN_RATE = 0.25
WEIGHT_DECAY = 0.1
COEF_A = 3.4445
COEF_B = -4.7750
COEF_C = 2.0315
NORM_EPS = 1e-7
NS_STEPS = 5

MESH = pl.DeviceIdType.MESH
SIDE = 4
PARTS = 3
STRIDES = (1, 4, 16)
JOINED = 5
LAST_KINDS = 4
KINDS = 6
CHUNKS = 3
GROUPS = (1, 1, 1)
LANES = 128
SPLIT = 40
SWAPS = 4
VMEM_KERNEL = 22 * 1024 * 1024
VMEM_FLUSH = 1024 * 1024
ORDER = (0, 3, 1, 2)


def dot_nn(lhs, rhs):
    return lax.dot_general(lhs, rhs, (((1,), (0,)), ((), ())), preferred_element_type=jnp.float32)


def dot_nt(lhs, rhs):
    return lax.dot_general(lhs, rhs, (((1,), (1,)), ((), ())), preferred_element_type=jnp.float32)


def over_rows(count, chunk, body):
    def run(index, carry):
        body(pl.ds(pl.multiple_of(index * chunk, chunk), chunk))
        return carry
    lax.fori_loop(0, count // chunk, run, 0)


def descend(weight_out, ortho_all, rms_scale, layer):
    def add(at):
        weight = weight_out[layer, at]
        ortho = ortho_all[layer, at].astype(jnp.float32)
        weight_out[layer, at] = weight - LEARN_RATE * (rms_scale * ortho + WEIGHT_DECAY * weight)

    over_rows(weight_out.shape[1], 48, add)


def kernel(rows, cols, data_size, rms_scale, grad_ref, mom_ref, weight_ref, held, ortho_all, x_buf, gram_buf, poly_buf,
           nest_in, send_sem, recv_sem, local_sem):
    data_idx = lax.axis_index("data")
    tp_idx = lax.axis_index("tp")
    partner = {"tp": 1 - tp_idx}
    half = rows // 2
    quarter = rows // SIDE
    eighth = quarter // 2
    layers = PARTS * SIDE
    mom_out = held.at[pl.ds(0, layers)]
    weight_out = held.at[pl.ds(layers, layers)]

    width = cols // CHUNKS

    def columns(chunk, start=0):
        return pl.ds(start + chunk * width, width)

    def raw_in(part, slot, chunk):
        return ortho_all.at[part * 3 + slot, :, columns(chunk)]

    def raw_relay(part, way, chunk):
        return ortho_all.at[3 * PARTS + part, pl.ds(way * half, half), columns(chunk)]

    def raw_own(part, chunk):
        return x_buf.at[part // 2, :, columns(chunk, part % 2 * cols)]

    def sum_line(part, chunk):
        return weight_out.at[part, :, columns(chunk)]

    def line_in(part, slot, chunk):
        return weight_out.at[PARTS + part, pl.ds(slot * quarter, quarter), columns(chunk)]

    def line_relay(part, way, chunk):
        return weight_out.at[PARTS + part, pl.ds(2 * quarter + way * eighth, eighth), columns(chunk)]

    block_rows = eighth

    def block_at(index, which, row, chunk):
        at = row + lax.div(index, 2) * block_rows + which * SPLIT
        size = block_rows - SPLIT if which else SPLIT
        lane = chunk * width + lax.rem(index, 2) * LANES
        return pl.ds(pl.multiple_of(at, 8), size), pl.ds(pl.multiple_of(lane, LANES), LANES)

    def plane(part, chunk):
        return weight_out.at[2 * PARTS + part, pl.ds(0, quarter), columns(chunk)]

    def plane_block(part, index, which, chunk):
        return weight_out.at[2 * PARTS + part, *block_at(index, which, 0, chunk)]

    def plane_in(part, slot, which, chunk):
        size = block_rows - SPLIT if which else SPLIT
        return weight_out.at[2 * PARTS + part, pl.ds(quarter + slot * block_rows + which * SPLIT, size),
                             pl.ds(chunk * width, LANES)]

    def plane_relay(part, way, chunk):
        size = block_rows - SPLIT if way else SPLIT
        return weight_out.at[2 * PARTS + part, pl.ds(quarter + way * SPLIT, size), pl.ds(chunk * width + LANES, LANES)]

    def mom_own(part):
        return weight_out.at[3 * PARTS + part]

    def nest(part):
        return weight_out.at[part]

    coord, plus, minus = [], [], []
    for stride in STRIDES:
        here = lax.rem(lax.div(data_idx, stride), SIDE)
        coord.append(here)
        plus.append({"data": data_idx + (lax.rem(here + 1, SIDE) - here) * stride})
        minus.append({"data": data_idx + (lax.rem(here + SIDE - 1, SIDE) - here) * stride})

    def step_of(axis, distance):
        return lax.rem(coord[axis] + distance, SIDE)

    def layer_of(part, distance):
        return part * SIDE + step_of(part, distance)

    def axes_of(part):
        return part, (part + 1) % PARTS, (part + 2) % PARTS

    def remote(src, dst, send, receive, device):
        return pltpu.make_async_remote_copy(src_ref=src, dst_ref=dst, send_sem=send_sem.at[send],
                                            recv_sem=recv_sem.at[receive], device_id=device, device_id_type=MESH)

    def numbers(phase, part, chunk, kind):
        group = chunk * PARTS + part
        send = phase % 2 * CHUNKS * PARTS + group
        later = JOINED * CHUNKS * PARTS * 2
        if phase < JOINED:
            return send, (phase * CHUNKS * PARTS + group) * 2 + (kind > 1)
        if phase == JOINED:
            return send, later + group * 2 + (kind > 1)
        return send, later + len(GROUPS) * PARTS * 2 + part * LAST_KINDS + (0, 0, 1, 2, 3, 3)[kind]

    def blocks(phase, chunk, count):
        if phase == 0:
            return ortho_all.at[pl.ds(0, count), :, columns(chunk)]
        if phase in (1, 4):
            return weight_out.at[0, pl.ds(0, count * quarter), columns(chunk)]
        if phase in (2, 3):
            return weight_out.at[0, pl.ds(0, count * block_rows), pl.ds(0, LANES)]
        if phase == 5:
            return mom_out.at[pl.ds(0, count), :, group_columns(chunk)]
        return ortho_all.at[pl.ds(0, count)]

    def await_blocks(phase, part, chunk, kind, count):
        landed = blocks(phase, chunk, count)
        remote(landed, landed, *numbers(phase, part, chunk, kind), partner).wait_recv()

    def relayed(phase, part, chunk=0):
        await_blocks(phase, part, chunk, 0, 1)

    def arrive(phase, part, chunk=0):
        await_blocks(phase, part, chunk, 2, 3 if phase == 0 else 2)

    def sent(phase, part, chunk=0):
        left = blocks(phase, chunk, 4 if phase == 0 else 3)
        remote(left, left, *numbers(phase, part, chunk, 2), partner).wait_send()

    def group_columns(group):
        return pl.ds(sum(GROUPS[:group]) * width, GROUPS[group] * width)

    def local(src, dst, index):
        return pltpu.make_async_copy(src, dst, local_sem.at[index])

    def spread(part, chunk):
        at_of = functools.partial(numbers, 0, part, chunk)
        far, right, left = layer_of(part, 2), layer_of(part, 1), layer_of(part, 3)

        def block(layer, at, size):
            return grad_ref.at[layer, pl.ds(at, size), columns(chunk)]

        def landing(slot, at, size):
            return raw_in(part, slot, chunk).at[pl.ds(at, size)]

        return [
            remote(block(far, 0, half), raw_relay(part, 0, chunk), *at_of(0), plus[part]),
            remote(block(far, half, half), raw_relay(part, 1, chunk), *at_of(1), minus[part]),
            remote(block(right, 0, rows), landing(0, 0, rows), *at_of(2), plus[part]),
            remote(block(left, 0, rows), landing(1, 0, rows), *at_of(3), minus[part]),
            remote(raw_relay(part, 0, chunk), landing(2, 0, half), *at_of(4), plus[part]),
            remote(raw_relay(part, 1, chunk), landing(2, half, half), *at_of(5), minus[part]),
        ]

    def line_block(part, distance, which, chunk):
        at = step_of(axes_of(part)[1], distance) * quarter + which * eighth
        return sum_line(part, chunk).at[pl.ds(pl.multiple_of(at, 8), eighth)]

    def reduce(phase, part, chunk, axis, block, relay, landing):
        at_of = functools.partial(numbers, phase, part, chunk)
        return [
            remote(block(2, 0), relay(0), *at_of(0), plus[axis]),
            remote(block(2, 1), relay(1), *at_of(1), minus[axis]),
            remote(block(1, 1), landing(0, 1), *at_of(2), plus[axis]),
            remote(block(3, 0), landing(1, 0), *at_of(3), minus[axis]),
            remote(relay(0), landing(0, 0), *at_of(4), plus[axis]),
            remote(relay(1), landing(1, 1), *at_of(5), minus[axis]),
        ]

    def relay_sums(copies, block, relay):
        for way, distance in ((0, 1), (1, 3)):
            into, own = relay(way), block(distance, way)

            def add(at, into=into, own=own):
                into[at] = into[at] + own[at]

            over_rows(into.shape[0], 8, add)
            copies[4 + way].start()

    def reduce_rows(part, chunk):
        def landing(slot, which):
            return line_in(part, slot, chunk).at[pl.ds(which * eighth, eighth)]

        return reduce(1, part, chunk, axes_of(part)[1], lambda distance, which: line_block(part, distance, which, chunk),
                      lambda way: line_relay(part, way, chunk), landing)

    def third_block(part, distance, which, chunk):
        return plane_block(part, step_of(axes_of(part)[2], distance), which, chunk)

    def reduce_blocks(part, chunk):
        return reduce(2, part, chunk, axes_of(part)[2], lambda distance, which: third_block(part, distance, which, chunk),
                      lambda way: plane_relay(part, way, chunk), lambda slot, which: plane_in(part, slot, which, chunk))

    def gather(phase, part, chunk, axis, slot):
        at_of = functools.partial(numbers, phase, part, chunk)
        here = coord[axis]
        left, right = step_of(axis, 3), step_of(axis, 1)
        return [
            remote(slot(here, 0), slot(here, 0), *at_of(0), plus[axis]),
            remote(slot(here, 1), slot(here, 1), *at_of(1), minus[axis]),
            remote(slot(here, 1), slot(here, 1), *at_of(2), plus[axis]),
            remote(slot(here, 0), slot(here, 0), *at_of(3), minus[axis]),
            remote(slot(left, 0), slot(left, 0), *at_of(4), plus[axis]),
            remote(slot(right, 1), slot(right, 1), *at_of(5), minus[axis]),
        ]

    def launch(copies):
        for copy in copies[:4]:
            copy.start()

    def forward(copies, *where):
        relayed(*where)
        copies[4].start()
        copies[5].start()

    fetch_raw, fetch_mom = [], []
    for part in range(PARTS):
        fetch_raw.append(local(grad_ref.at[layer_of(part, 0)], x_buf.at[part // 2, :, pl.ds(part % 2 * cols, cols)], part))
        fetch_mom.append(local(mom_ref.at[layer_of(part, 0)], mom_own(part), PARTS + part))
    for fetch in fetch_raw + fetch_mom:
        fetch.start()

    barrier = pltpu.get_barrier_semaphore()
    for device in plus + minus + [partner]:
        pl.semaphore_signal(barrier, inc=1, device_id=device, device_id_type=MESH)
    pl.semaphore_wait(barrier, 2 * PARTS + 1)

    chunks, parts = range(CHUNKS), range(PARTS)
    copies1 = [[spread(part, chunk) for part in parts] for chunk in chunks]
    copies2 = [[reduce_rows(part, chunk) for part in parts] for chunk in chunks]
    copies3 = [[reduce_blocks(part, chunk) for part in parts] for chunk in chunks]
    copies4, copies5, copies6, copies7 = ({}, {}, {}, {})

    def sum_raw(part, chunk):
        arrive(0, part, chunk)
        own, into = raw_own(part, chunk), sum_line(part, chunk)
        first, second, third = (raw_in(part, slot, chunk) for slot in range(3))

        def add(at):
            total = own[at].astype(jnp.float32) + first[at].astype(jnp.float32)
            into[at] = (total + second[at].astype(jnp.float32)) + third[at].astype(jnp.float32)

        over_rows(rows, 48, add)
        launch(copies2[chunk][part])

    def relay_rows(part, chunk):
        relayed(1, part, chunk)
        relay_sums(copies2[chunk][part], lambda distance, way: line_block(part, distance, way, chunk),
                   lambda way: line_relay(part, way, chunk))

    def sum_rows(part, chunk):
        arrive(1, part, chunk)
        into = plane(part, chunk)
        for which in range(2):
            own = line_block(part, 0, which, chunk)

            def add(at, own=own, which=which):
                row = pl.ds(pl.multiple_of(which * eighth + at.start, 8), at.size)
                into[row] = own[at] + (line_in(part, 0, chunk)[row] + line_in(part, 1, chunk)[row])

            over_rows(eighth, 24, add)
        sent(0, part, chunk)
        launch(copies3[chunk][part])

    def relay_blocks(part, chunk):
        relayed(2, part, chunk)
        relay_sums(copies3[chunk][part], lambda distance, way: third_block(part, distance, way, chunk),
                   lambda way: plane_relay(part, way, chunk))

    def sum_blocks(part, chunk):
        arrive(2, part, chunk)
        axis_b, axis_c = axes_of(part)[1:]
        layer = layer_of(part, 0)

        def slot(index, which):
            return mom_out.at[layer, *block_at(index, which, coord[axis_b] * quarter, chunk)]

        for which in range(2):
            into, own = slot(coord[axis_c], which), third_block(part, 0, which, chunk)
            first, second = plane_in(part, 0, which, chunk), plane_in(part, 1, which, chunk)

            def add(at, into=into, own=own, first=first, second=second):
                into[at] = (own[at] + (first[at] + second[at])) * (1.0 / data_size)

            over_rows(own.shape[0], 8, add)
        sent(1, part, chunk)
        copies4[chunk, part] = gather(3, part, chunk, axis_c, slot)
        launch(copies4[chunk, part])

    def gather_rows(part, chunk):
        arrive(3, part, chunk)
        layer = layer_of(part, 0)

        def slot(index, which):
            return mom_out.at[layer, pl.ds(pl.multiple_of(index * quarter + which * eighth, 8), eighth), columns(chunk)]

        sent(2, part, chunk)
        copies5[chunk, part] = gather(4, part, chunk, axes_of(part)[1], slot)
        launch(copies5[chunk, part])

    def gather_means(part, chunk):
        arrive(4, part, chunk)
        ends = [sum(GROUPS[:group + 1]) - 1 for group in range(len(GROUPS))]
        if chunk not in ends:
            return
        group = ends.index(chunk)

        def slot(index, which):
            return mom_out.at[part * SIDE + index, pl.ds(which * half, half), group_columns(group)]

        sent(3, part, group)
        copies6[group, part] = gather(5, part, group, part, slot)
        for copy in copies6[group, part][:2]:
            copy.start()

    for part in parts:
        launch(copies1[0][part])

    def ahead(chunk, kinds):
        if chunk < CHUNKS:
            for part in parts:
                for kind in kinds:
                    copies1[chunk][part][kind].start()

    def forward_raw(part, chunk):
        if part == 0 and chunk == 0:
            ahead(1, (0, 1))
        forward(copies1[chunk][part], 0, part, chunk)
        if part == PARTS - 1:
            ahead(chunk + 1, (2, 3))
            ahead(chunk + 2, (0, 1))

    for part in parts:
        fetch_raw[part].wait()
    stages = [
        forward_raw,
        sum_raw,
        relay_rows,
        sum_rows,
        relay_blocks,
        sum_blocks,
        lambda part, chunk: forward(copies4[chunk, part], 3, part, chunk),
        gather_rows,
        lambda part, chunk: forward(copies5[chunk, part], 4, part, chunk),
        gather_means,
    ]
    for tick in range(len(stages) + CHUNKS - 1):
        for chunk in reversed(chunks):
            if 0 <= tick - chunk < len(stages):
                for part in parts:
                    stages[tick - chunk](part, chunk)
    groups = range(len(GROUPS))
    for group in groups:
        for part in parts:
            for copy in copies6[group, part][2:4]:
                copy.start()
    for part in parts:
        for group in range(len(GROUPS), CHUNKS):
            sent(3, part, group)

    swap_send, swap_receive = 2 * CHUNKS * PARTS, JOINED * CHUNKS * PARTS * 2 + PARTS * (len(GROUPS) * 2 + LAST_KINDS)
    for part in range(PARTS):
        fetch_mom[part].wait()

        def nesterov(at, part=part):
            mean = mom_out[layer_of(part, 0), at]
            nest(part)[at] = mean + MOMENTUM * (MOMENTUM * mom_own(part)[at] + mean)

        over_rows(rows, 16, nesterov)
    give_first = remote(weight_out.at[1 - tp_idx], nest_in.at[0], swap_send + 0, swap_receive + 0, partner)
    give_first.start()
    give_second = remote(nest(2), nest_in.at[1], swap_send + 1, swap_receive + 1, partner)

    @pl.when(tp_idx == 1)
    def _():
        give_second.start()

    weight_base = 2 * PARTS
    fetch_weight = [local(weight_ref.at[layer], weight_out.at[layer], weight_base) for layer in range(layers)]
    for fetch in fetch_weight[PARTS:]:
        fetch.start()

    def orthogonalise(part, which, ready=None):
        def squares(index, total):
            at = pl.ds(pl.multiple_of(index * 8, 8), 8)
            own, other = weight_out[part, at], nest_in[which, at]
            return total + (own * own + other * other)

        total = lax.fori_loop(0, rows // 8, squares, jnp.zeros((8, cols), jnp.float32))
        scale = 1.0 / (jnp.sqrt(jnp.sum(total, keepdims=True)) + NORM_EPS)

        def normalise(at):
            x_buf[0, at, pl.ds(0, cols)] = (weight_out[part, at] * scale).astype(jnp.bfloat16)
            x_buf[0, at, pl.ds(cols, cols)] = (nest_in[which, at] * scale).astype(jnp.bfloat16)

        over_rows(rows, 16, normalise)
        if ready is not None:
            ready()

        def newton(step, carry):
            now = lax.rem(step, 2)
            later = 1 - now
            gram_buf[...] = dot_nt(x_buf[now], x_buf[now]).astype(jnp.bfloat16)
            square = dot_nn(gram_buf[...], gram_buf[...])
            poly_buf[...] = (COEF_B * gram_buf[...].astype(jnp.float32) + COEF_C * square).astype(jnp.bfloat16)
            for at in range(0, 2 * cols, cols // 3):
                strip = x_buf[now, :, pl.ds(at, cols // 3)]
                update = dot_nn(poly_buf[...], strip)
                x_buf[later, :, pl.ds(at, cols // 3)] = (COEF_A * strip.astype(jnp.float32) + update).astype(jnp.bfloat16)
            return carry

        lax.fori_loop(0, NS_STEPS, newton, 0)

    final = NS_STEPS % 2
    first_layer = jnp.where(tp_idx == 0, layer_of(0, 0), layer_of(1, 0))

    def keep_half(layer):
        def move(at):
            ortho_all[layer, at] = x_buf[final, at, pl.ds(0, cols)]
        over_rows(rows, 16, move)

    for part in parts:
        def slot(index, which, part=part):
            return ortho_all.at[part * SIDE + index, pl.ds(which * half, half)]

        copies7[part] = gather(6, part, 0, part, slot)

    give_first.wait_recv()
    orthogonalise(tp_idx, 0)
    swap_x = remote(x_buf.at[final, :, pl.ds(cols, cols)], ortho_all.at[first_layer], swap_send + 2, swap_receive + 2, partner)
    swap_x.start()
    for group in groups:
        for part in parts:
            forward(copies6[group, part], 5, part, group)
    keep_half(first_layer)
    for chunk in chunks:
        for part in parts:
            sent(4, part, chunk)
    give_x = remote(x_buf.at[final, :, pl.ds(cols, cols)], ortho_all.at[layer_of(2, 0)], swap_send + 3, swap_receive + 3, partner)

    @pl.when(tp_idx == 0)
    def _():
        launch(copies7[0])
        give_second.wait_recv()
        orthogonalise(2, 1, swap_x.wait_send)
        give_x.start()
        keep_half(layer_of(2, 0))
        launch(copies7[2])
        swap_x.wait_recv()
        launch(copies7[1])
        give_x.wait_send()

    @pl.when(tp_idx == 1)
    def _():
        launch(copies7[1])
        swap_x.wait()
        launch(copies7[0])
        give_x.wait_recv()
        launch(copies7[2])
        give_second.wait_send()

    give_first.wait_send()
    for fetch in fetch_weight[:PARTS]:
        fetch.start()

    stream_base = weight_base + 1
    turns = [(part, distance) for distance in ORDER for part in range(PARTS)]
    fetch_turn = [local(mom_ref.at[layer_of(*turn)], nest_in.at[index % 2], stream_base + index % 2)
                  for index, turn in enumerate(turns)]
    fetch_turn[0].start()
    fetch_turn[1].start()
    for index, (part, distance) in enumerate(turns):
        for group in groups:
            if distance == 0:
                sent(5, part, group)
            elif distance == 3:
                arrive(5, part, group)
        fetch_turn[index].wait()
        layer = layer_of(part, distance)

        def momentum(at, layer=layer, index=index):
            mom_out[layer, at] = MOMENTUM * nest_in[index % 2, at] + mom_out[layer, at]

        over_rows(rows, 16, momentum)
        if index + 2 < len(turns):
            fetch_turn[index + 2].start()

    for part in range(PARTS):
        forward(copies7[part], 6, part)
    local(weight_ref, weight_out, weight_base).wait()
    for part, distance in turns:
        if distance == 3:
            copies7[part][2].wait_recv()
        elif distance == 1:
            copies7[part][3].wait_recv()
        elif distance == 2:
            await_blocks(6, part, 0, 4, 1)
        descend(weight_out, ortho_all, rms_scale, layer_of(part, distance))
    for part in parts:
        sent(6, part)


def flush(held, mom_ref, weight_ref, sem):
    layers = mom_ref.shape[0]
    mom_out = held.at[pl.ds(0, layers)]
    weight_out = held.at[pl.ds(layers, layers)]
    for layer in range(layers):
        pltpu.make_async_copy(mom_out.at[layer], mom_ref.at[layer], sem.at[0]).start()
        pltpu.make_async_copy(weight_out.at[layer], weight_ref.at[layer], sem.at[1]).start()
    pltpu.make_async_copy(mom_out, mom_ref, sem.at[0]).wait()
    pltpu.make_async_copy(weight_out, weight_ref, sem.at[1]).wait()


def solution(mesh):
    data_size = mesh.shape["data"]
    tp_size = mesh.shape["tp"]
    state_spec = P("stage", None, "tp")
    grad_spec = P("stage", "data", None, "tp")

    def per_device(weight, momentum, grad):
        layers, rows, cols = weight.shape
        sends = 2 * CHUNKS * PARTS + SWAPS
        receives = JOINED * CHUNKS * PARTS * 2 + PARTS * (len(GROUPS) * 2 + LAST_KINDS) + SWAPS
        rms_scale = 0.2 * math.sqrt(max(rows, cols * tp_size))
        bf16, f32 = jnp.bfloat16, jnp.float32
        in_hbm = pl.BlockSpec(memory_space=pltpu.HBM)
        in_vmem = pl.BlockSpec(memory_space=pltpu.VMEM)
        held = pl.pallas_call(
            functools.partial(kernel, rows, cols, data_size, rms_scale),
            out_shape=pltpu.VMEM((2 * layers, rows, cols), f32),
            in_specs=[in_hbm] * 3,
            out_specs=in_vmem,
            scratch_shapes=[
                pltpu.VMEM((layers, rows, cols), bf16),
                pltpu.VMEM((2, rows, tp_size * cols), bf16),
                pltpu.VMEM((rows, rows), bf16),
                pltpu.VMEM((rows, rows), bf16),
                pltpu.VMEM((2, rows, cols), f32),
                pltpu.SemaphoreType.DMA((sends,)),
                pltpu.SemaphoreType.DMA((receives,)),
                pltpu.SemaphoreType.DMA((2 * PARTS + 3,)),
            ],
            compiler_params=pltpu.CompilerParams(collective_id=0, has_side_effects=True, vmem_limit_bytes=VMEM_KERNEL),
        )(grad.reshape(layers, rows, cols), momentum, weight)
        new_mom, new_weight = pl.pallas_call(
            flush,
            out_shape=(jax.ShapeDtypeStruct((layers, rows, cols), f32),) * 2,
            in_specs=[in_vmem],
            out_specs=(in_hbm,) * 2,
            scratch_shapes=[pltpu.SemaphoreType.DMA((2,))],
            compiler_params=pltpu.CompilerParams(vmem_limit_bytes=VMEM_FLUSH),
        )(held)
        return new_weight, new_mom

    return jax.shard_map(per_device, mesh=mesh, in_specs=(state_spec, state_spec, grad_spec), out_specs=(state_spec, state_spec), check_vma=False)
```
